32 devices in a mesh: len: 2 (over x), tile: 16 (over z, y, core).
Axes of the slice: x: 2, y: 2, z: 4, core: 2. Of those that a mesh axis runs over, the one named last changes fastest.
Arguments:
- series: float32 [9216], P('tile'), may hold values from -24 to 24
- window_lengths: int32 [4], P('len'), may hold values from 64 to 1024, as said below
- exclusion: int32 [4], P('len'), may hold values from 16 to 256
- tile_list: int32 [64, 2], P('tile'), may hold values from 0 to 15, as said below
Outputs:
- right_profile: float32 [4, 8192], P(None, 'tile')
- left_profile: float32 [4, 8192], P(None, 'tile')
The draws below stay inside these ranges and needn't reach their ends.
Inputs may be any that keep to these rules, and one draw needn't show every extreme that they name: `window_lengths`: the largest is exactly 1024. `tile_list`: each row is a pair (row block, column block) with row block <= column block; no pair appears twice.
All inputs are finite; a program needn't handle non-finite values.
Results may differ from the reference program's by a relative error of at most 0.00039.
Values sent between devices are 32-bit elements; how exact they have to be, the bound alone decides.
A program may use at most 64 MiB of HBM per device.

```python
import jax
import jax.numpy as jnp
from jax import lax

MIN_LEN = 64
OCTAVES = 4
MAX_LEN = 1024
LENGTHS = 4
TILE_SIDE = 512
COL_BLOCK = 512
TILE_ROWS = 16
SERIES_LENGTH = 9216
TILE_SLOTS = 64


def draw_series(key, part):
    noise_key, wave_key, phase_key = jax.random.split(key, 3)
    sample_times = jnp.arange(SERIES_LENGTH, dtype=jnp.float32)
    wave_frequencies = jax.random.uniform(wave_key, (4,), jnp.float32, 0.002, 0.05)
    wave_phases = jax.random.uniform(phase_key, (4,), jnp.float32, -3.14159, 3.14159)
    smoothed_series = 0.5 * jnp.sum(jnp.sin(sample_times[:, None] * wave_frequencies[None, :] + wave_phases[None, :]), axis=1)
    jitter = jnp.clip(jax.random.normal(noise_key, (SERIES_LENGTH,), jnp.float32), -6.0, 6.0)
    return jitter + smoothed_series


def draw_window_lengths(key, part):
    octave_key, offset_key, pick_key = jax.random.split(key, 3)
    octave = jax.random.randint(octave_key, (LENGTHS,), 0, OCTAVES)
    lowest = MIN_LEN * jnp.left_shift(jnp.ones((LENGTHS,), jnp.int32), octave.astype(jnp.int32))
    surplus = jax.random.randint(offset_key, (LENGTHS,), 0, 1 << 30) % (lowest + 1)
    chosen = jax.random.randint(pick_key, (), 0, LENGTHS)
    lengths = jnp.where(jnp.arange(LENGTHS) == chosen, MAX_LEN, lowest + surplus)
    return lengths.astype(jnp.int32)


def draw_tile_list(key, part):
    grid_rows = lax.broadcasted_iota(jnp.int32, (TILE_ROWS, TILE_ROWS), 0)
    grid_cols = lax.broadcasted_iota(jnp.int32, (TILE_ROWS, TILE_ROWS), 1)
    upper = (grid_rows <= grid_cols).reshape(-1)
    triangle = TILE_ROWS * (TILE_ROWS + 1) // 2
    flat_ids = jnp.nonzero(upper, size=triangle)[0].astype(jnp.int32)
    order = jax.random.permutation(key, triangle)[:TILE_SLOTS]
    picked = flat_ids[order]
    return jnp.stack([picked // TILE_ROWS, picked % TILE_ROWS], axis=1).astype(jnp.int32)


def place_ends(result, stream_key, low, largest):
    spot = [jax.random.randint(jax.random.fold_in(stream_key, axis), (), 0, length) for axis, length in enumerate(result.shape)]
    longest = result.shape.index(max(result.shape))
    neighbour = spot[:longest] + [(spot[longest] + 1) % result.shape[longest]] + spot[longest + 1:]
    return result.at[tuple(spot)].set(low).at[tuple(neighbour)].set(largest)


def setup_inputs(seed: int = 0) -> dict:
    keys = jax.random.split(jax.random.key(seed), 5)
    series = draw_series(jax.random.fold_in(keys[4], 71), 0)
    window_lengths = draw_window_lengths(jax.random.fold_in(keys[4], 71), 0)
    exclusion = place_ends(jax.random.randint(keys[2], (LENGTHS,), MIN_LEN // 4, MAX_LEN // 4 + 1), jax.random.fold_in(keys[2], 1), MIN_LEN // 4, (MAX_LEN // 4 + 1) - 1).astype(jnp.int32)
    tile_list = draw_tile_list(jax.random.fold_in(keys[4], 71), 0)
    return {"series": series, "window_lengths": window_lengths, "exclusion": exclusion, "tile_list": tile_list}


EMPTY_VALUE = 2.0
VAR_EPS = 1e-05

def shifted_block(segment, offset, columns, positions):
    window = lax.dynamic_slice_in_dim(segment, offset, positions + columns)
    stride = positions + columns + 1
    repeated = jnp.tile(window, columns + 1)[:columns * stride]
    return repeated.reshape(columns, stride)[:, :positions]

def window_stats(segment, length, positions, columns):
    blocks = (length + columns - 1) // columns
    col_ids = lax.broadcasted_iota(jnp.int32, (columns, 1), 0)
    denominator = length.astype(jnp.float32)
    initial = jnp.zeros((positions,), jnp.float32)

    def add_sum(part_index, running):
        values = shifted_block(segment, part_index * columns, columns, positions)
        inside = col_ids + part_index * columns < length
        return running + lax.optimization_barrier(jnp.sum(jnp.where(inside, values, 0.0), axis=0))
    centre = lax.fori_loop(0, blocks, add_sum, initial) / denominator

    def add_square(part_index, running):
        values = shifted_block(segment, part_index * columns, columns, positions) - centre[None, :]
        inside = col_ids + part_index * columns < length
        return running + lax.optimization_barrier(jnp.sum(jnp.where(inside, values * values, 0.0), axis=0))
    spread = lax.fori_loop(0, blocks, add_square, initial) / denominator
    return (centre, 1.0 / jnp.sqrt(spread + VAR_EPS))

def normalized(segment, part_index, centre, inverse, length):
    values = shifted_block(segment, part_index * COL_BLOCK, COL_BLOCK, TILE_SIDE)
    col_ids = lax.broadcasted_iota(jnp.int32, (COL_BLOCK, 1), 0)
    inside = col_ids + part_index * COL_BLOCK < length
    return jnp.where(inside, (values - centre[None, :]) * inverse[None, :], 0.0).astype(jnp.bfloat16)

def tile_minima(row_segment, col_segment, row_stats, col_stats, length, barrier, row_start, col_start):
    blocks = (length + COL_BLOCK - 1) // COL_BLOCK

    def add_block(part_index, running):
        row_normal = normalized(row_segment, part_index, row_stats[0], row_stats[1], length).astype(jnp.float32)
        col_normal = normalized(col_segment, part_index, col_stats[0], col_stats[1], length).astype(jnp.float32)
        return running + lax.dot_general(row_normal, col_normal, (((0,), (0,)), ((), ())), precision=lax.Precision.HIGHEST, preferred_element_type=jnp.float32)
    product = lax.fori_loop(0, blocks, add_block, jnp.zeros((TILE_SIDE, TILE_SIDE), jnp.float32))
    distance = 1.0 - product / length.astype(jnp.float32)
    row_ids = row_start + lax.broadcasted_iota(jnp.int32, (TILE_SIDE, 1), 0)
    col_ids = col_start + lax.broadcasted_iota(jnp.int32, (1, TILE_SIDE), 1)
    distance = jnp.where(col_ids - row_ids > barrier, distance, EMPTY_VALUE)
    return (lax.optimization_barrier(jnp.min(distance, axis=1)), lax.optimization_barrier(jnp.min(distance, axis=0)))

def reference(series, window_lengths, exclusion, tile_list):
    positions = TILE_ROWS * TILE_SIDE
    block_ids = jnp.arange(TILE_ROWS, dtype=jnp.int32)

    def one_length(setting):
        length, barrier = setting

        def stats_block(row_block):
            segment = lax.dynamic_slice_in_dim(series, row_block * TILE_SIDE, TILE_SIDE + MAX_LEN)
            return window_stats(segment, length, TILE_SIDE, COL_BLOCK)
        centres, inverses = lax.map(stats_block, block_ids)
        centres = centres.reshape(positions)
        inverses = inverses.reshape(positions)

        def one_tile(profiles, tile_pair):
            right_lowest_distance, left_best = profiles
            row_start = (tile_pair[0] * TILE_SIDE).astype(jnp.int32)
            col_start = (tile_pair[1] * TILE_SIDE).astype(jnp.int32)
            row_segment = lax.dynamic_slice_in_dim(series, row_start, TILE_SIDE + MAX_LEN)
            col_segment = lax.dynamic_slice_in_dim(series, col_start, TILE_SIDE + MAX_LEN)
            row_stats = (lax.dynamic_slice_in_dim(centres, row_start, TILE_SIDE), lax.dynamic_slice_in_dim(inverses, row_start, TILE_SIDE))
            col_stats = (lax.dynamic_slice_in_dim(centres, col_start, TILE_SIDE), lax.dynamic_slice_in_dim(inverses, col_start, TILE_SIDE))
            right_min, left_min = tile_minima(row_segment, col_segment, row_stats, col_stats, length, barrier, row_start, col_start)
            right_old = lax.dynamic_slice_in_dim(right_lowest_distance, row_start, TILE_SIDE)
            right_lowest_distance = lax.dynamic_update_slice_in_dim(right_lowest_distance, jnp.minimum(right_old, right_min), row_start, 0)
            left_old = lax.dynamic_slice_in_dim(left_best, col_start, TILE_SIDE)
            left_best = lax.dynamic_update_slice_in_dim(left_best, jnp.minimum(left_old, left_min), col_start, 0)
            return ((right_lowest_distance, left_best), None)
        blank = jnp.full((positions,), EMPTY_VALUE, jnp.float32)
        profiles, leftover = lax.scan(one_tile, (blank, blank), tile_list)
        return profiles
    right_lowest_distance, left_best = lax.map(one_length, (window_lengths, exclusion))
    return (right_lowest_distance, left_best)
```

```python
import functools

import jax
import jax.numpy as jnp
from jax import lax
from jax.experimental import pallas as pl
from jax.experimental.pallas import tpu as pltpu
from jax.sharding import PartitionSpec as P

MAX_LEN = 1024
TILE_SIDE = 512
LANES = 128
SUBLANES = 8
GRANT = 1 << 20
QUARTERS = TILE_SIDE // LANES

VAR_EPS = 1e-05

VMEM = pltpu.MemorySpace.VMEM
SMEM = pltpu.MemorySpace.SMEM
HBM = pltpu.MemorySpace.HBM


def partner(me, step, n):
    if n & (n - 1):
        return lax.rem(me + step, n)
    peer = me
    for b in range(n.bit_length() - 1):
        if step >> b & 1:
            peer = peer + (1 << b) * (1 - 2 * lax.rem(lax.div(me, 1 << b), 2))
    return peer


def steps_of(n):
    return range(n - 1, 0, -1)


def signal_all(barrier, axis, n):
    me = lax.axis_index(axis)
    for step in range(1, n) if n & (n - 1) else steps_of(n):
        pl.semaphore_signal(
            barrier,
            inc=1,
            device_id={axis: partner(me, step, n)},
            device_id_type=pl.DeviceIdType.MESH,
        )


def copy_to(axis, n, step, source, target, send_sem, recv_sem):
    return pltpu.make_async_remote_copy(
        src_ref=source,
        dst_ref=target,
        send_sem=send_sem,
        recv_sem=recv_sem,
        device_id={axis: partner(lax.axis_index(axis), step, n)},
        device_id_type=pl.DeviceIdType.MESH,
    )


def shifted(values, count):
    rows = values.shape[0]
    skip, shift = count // LANES, count % LANES
    if shift:
        lane_ids = lax.broadcasted_iota(jnp.int32, values.shape, 1)
        values = pltpu.roll(values, LANES - shift, 1)
        values = jnp.where(lane_ids < LANES - shift, values, pltpu.roll(values, rows - 1, 0))
    if skip:
        values = pltpu.roll(values, rows - skip, 0)
    return values


def window_stats(packed, lengths):
    mean, spread = packed, jnp.zeros_like(packed)
    results = [(jnp.zeros_like(packed), jnp.zeros_like(packed)) for _ in lengths]
    bits = MAX_LEN.bit_length()
    for b in range(bits):
        first = 1 << b
        for l, length in enumerate(lengths):
            tail_mean, tail_spread = results[l]
            if b:
                tail_mean, tail_spread = shifted(tail_mean, first), shifted(tail_spread, first)
            rest = lax.rem(length, first).astype(jnp.float32)
            share = rest / (rest + first)
            gap = tail_mean - mean
            taken = (jnp.full(packed.shape, length) & first) != 0
            results[l] = (
                jnp.where(taken, mean + gap * share, results[l][0]),
                jnp.where(
                    taken, spread + tail_spread + gap * gap * (share * first), results[l][1]
                ),
            )
        if b < bits - 1:
            next_mean = shifted(mean, first)
            gap = next_mean - mean
            mean = 0.5 * (mean + next_mean)
            if b:
                spread = spread + shifted(spread, first) + gap * gap * (0.5 * first)
            else:
                spread = gap * gap * 0.5
    return [
        (mean, 1.0 / jnp.sqrt(spread / length.astype(jnp.float32) + VAR_EPS))
        for (mean, spread), length in zip(results, lengths)
    ]


def profile_kernel(
    piece,
    n,
    count_len,
    len_devices,
    slots_of_tiles,
    series_ref,
    tile_hbm,
    length_hbm,
    barrier_hbm,
    groups,
    piece_ref,
    tile_ref,
    length_ref,
    barrier_ref,
    flat,
    staged,
    slots,
    packed,
    base,
    centre_ref,
    inverse_ref,
    keep_ref,
    left_op,
    right_op,
    best,
    parts,
    mine,
    in_sem,
    send_piece,
    recv_piece,
    send_sem,
    recv_sem,
    send_len,
    recv_len,
):
    me = lax.axis_index("tile")
    my_len = lax.axis_index("len")
    loads = [
        pltpu.make_async_copy(source, target, in_sem.at[k])
        for k, (source, target) in enumerate(
            (
                (series_ref, piece_ref),
                (tile_hbm, tile_ref),
                (length_hbm, length_ref),
                (barrier_hbm, barrier_ref),
            )
        )
    ]
    loads[0].start()
    barrier = pltpu.get_barrier_semaphore()
    signal_all(barrier, "tile", n)
    signal_all(barrier, "len", len_devices)
    for load in loads[1:]:
        load.start()

    slot_rows = staged.shape[0]
    flat[...] = jnp.zeros(flat.shape, jnp.float32)
    loads[0].wait()
    flat[:piece] = piece_ref[...]
    values = flat[...].reshape(slot_rows, LANES)
    shift = lax.rem(me * piece, LANES)
    lane_ids = lax.broadcasted_iota(jnp.int32, values.shape, 1)
    values = pltpu.roll(values, shift, 1)
    staged[...] = jnp.where(lane_ids >= shift, values, pltpu.roll(values, 1, 0))

    pl.semaphore_wait(barrier, n - 1 + len_devices - 1)
    copies = [
        copy_to("tile", n, step, staged, slots.at[me], send_piece.at[step], recv_piece.at[step])
        for step in steps_of(n)
    ]
    for copy in copies:
        copy.start()
    slots[me] = staged[...]
    for load in loads[1:]:
        load.wait()

    lengths = [length_ref[l] for l in range(count_len)]
    row_ids = lax.broadcasted_iota(jnp.int32, (MAX_LEN, LANES), 0)
    row_ids = row_ids + (SUBLANES - 1) - 2 * lax.rem(row_ids, SUBLANES)
    for l, length in enumerate(lengths):
        keep_ref[l] = jnp.where(row_ids < length, 1.0, 0.0).astype(jnp.bfloat16)
        best[l] = jnp.full(best.shape[1:], -length.astype(jnp.float32), jnp.float32)
    packed[...] = jnp.zeros(packed.shape, jnp.float32)
    for copy in copies:
        copy.wait_recv()

    columns = packed.shape[0]
    for t in range(n):
        low, first = divmod(t * piece, LANES)
        used = (first + piece + LANES - 1) // LANES
        packed[low : low + used, :] += slots[t, :used, :]

    for l, (centre, inverse) in enumerate(window_stats(packed[...], lengths)):
        centre_ref[l] = centre.reshape(columns, 1, LANES)
        inverse_ref[l] = inverse.reshape(columns, 1, LANES)

    sub = lax.broadcasted_iota(jnp.int32, (SUBLANES, LANES), 0)
    lane = lax.broadcasted_iota(jnp.int32, (SUBLANES, LANES), 1)
    groups8 = LANES // SUBLANES
    span = 12 if columns % 12 == 0 else 1

    def spread_columns(k, turned):
        for j in range(span):
            a = columns - 1 - k * span - j
            row = jnp.broadcast_to(packed[pl.ds(a, 1), :], (SUBLANES, LANES))
            later = []
            for g in range(groups8):
                moved = pltpu.roll(row, LANES + 1 - SUBLANES * (g + 1), 1, stride=1, stride_axis=0)
                base[a, SUBLANES * g : SUBLANES * (g + 1), :] = jnp.where(
                    lane - sub < LANES + 1 - SUBLANES * (g + 1), moved, turned[g]
                )
                later.append(moved)
            turned = tuple(later)
        return turned

    lax.fori_loop(
        0,
        columns // span,
        spread_columns,
        (jnp.zeros((SUBLANES, LANES), jnp.float32),) * groups8,
    )

    def build(l, slot, buffer):
        firsts = [tile_ref[k, slot] * QUARTERS for k in range(2)]
        for k, (first, target) in enumerate(zip(firsts, (left_op, right_op))):
            for u in range(QUARTERS):
                centre, inverse = centre_ref[l, first + u], inverse_ref[l, first + u]
                for c in range(MAX_LEN // LANES):
                    rows = slice(c * LANES, (c + 1) * LANES)
                    normal = ((base[first + u + c] - centre) * inverse).astype(jnp.bfloat16)
                    if k == 0:
                        normal = normal * keep_ref[l, rows, :]
                    target[buffer, rows, u * LANES : (u + 1) * LANES] = normal

    def product(l, slot, buffer):
        row_block, col_block = tile_ref[0, slot], tile_ref[1, slot]
        size = lengths[l].astype(jnp.float32)
        limit = barrier_ref[l] - (col_block - row_block) * TILE_SIDE
        tops = [None] * QUARTERS
        found = []
        for low in range(0, TILE_SIDE, 2 * LANES):
            values = lax.dot_general(
                left_op[buffer, :, low : low + 2 * LANES],
                right_op[buffer],
                (((0,), (0,)), ((), ())),
                preferred_element_type=jnp.float32,
            )
            ahead = lax.broadcasted_iota(jnp.int32, values.shape, 1) - (
                lax.broadcasted_iota(jnp.int32, values.shape, 0) + low
            )
            values = jnp.where(ahead > limit, values, -size)
            folded = None
            for u in range(QUARTERS):
                part = values[:, u * LANES : (u + 1) * LANES]
                folded = part if folded is None else jnp.maximum(folded, part)
                top = jnp.max(part, axis=0, keepdims=True)
                tops[u] = top if tops[u] is None else jnp.maximum(tops[u], top)
            for q in range(2):
                turned_back = jnp.transpose(folded[q * LANES : (q + 1) * LANES, :])
                found.append(jnp.max(turned_back, axis=0, keepdims=True))
        both = jnp.full((SUBLANES, LANES), -size, jnp.float32)
        for u in range(QUARTERS):
            both = jnp.where(sub == u, found[u], both)
            both = jnp.where(sub == QUARTERS + u, tops[u], both)
        row_is, col_is = jnp.full(sub.shape, row_block), jnp.full(sub.shape, col_block)
        owner = jnp.where(sub < QUARTERS, row_is, col_is)
        for b in range(n):
            old = best[l, b]
            best[l, b] = jnp.where(owner == b, jnp.maximum(old, both), old)

    sends = []
    work = [(l, slot) for l in range(count_len) for slot in range(slots_of_tiles)]
    build(*work[0], 0)
    for p, (l, slot) in enumerate(work):
        if p + 1 < len(work):
            build(*work[p + 1], (p + 1) % 2)
        product(l, slot, p % 2)
        if slot == slots_of_tiles - 1:
            sends.append(
                [
                    copy_to(
                        "tile",
                        n,
                        step,
                        best.at[l, partner(me, step, n)],
                        parts.at[l, step],
                        send_sem.at[l, step],
                        recv_sem.at[l, step],
                    )
                    for step in steps_of(n)
                ]
            )
            for copy in sends[-1]:
                copy.start()

    for l in range(count_len):
        for copy in sends[l]:
            copy.wait_recv()
        merged = best[l, me]
        for step in range(1, n):
            merged = jnp.maximum(merged, parts[l, step])
        merged = 1.0 - merged / lengths[l].astype(jnp.float32)
        mine[l] = merged
        groups[my_len, l] = merged
    copies_len = [
        copy_to("len", len_devices, step, mine, groups.at[my_len], send_len.at[step], recv_len.at[step])
        for step in range(1, len_devices)
    ]
    for copy in copies_len:
        copy.start()
    for copy in copies:
        copy.wait_send()
    for some in sends:
        for copy in some:
            copy.wait_send()
    for copy in copies_len:
        copy.wait()


def write_kernel(groups_ref, right_ref, left_ref, right, left, sems):
    len_devices, count_len = groups_ref.shape[:2]
    for g in range(len_devices):
        for l in range(count_len):
            row = g * count_len + l
            for u in range(QUARTERS):
                lanes = slice(u * LANES, (u + 1) * LANES)
                right[row : row + 1, lanes] = groups_ref[g, l, u : u + 1, :]
                left[row : row + 1, lanes] = groups_ref[g, l, QUARTERS + u : QUARTERS + u + 1, :]
    copies = [
        pltpu.make_async_copy(right, right_ref, sems.at[0]),
        pltpu.make_async_copy(left, left_ref, sems.at[1]),
    ]
    for copy in copies:
        copy.start()
    for copy in copies:
        copy.wait()


def shards(series, window_lengths, exclusion, tile_list):
    n = lax.axis_size("tile")
    len_devices = lax.axis_size("len")
    count_len = window_lengths.shape[0]
    piece = series.shape[0]
    points = piece * n
    columns = points // LANES
    blocks = (points - MAX_LEN) // TILE_SIDE
    assert blocks == n
    slot_rows = (piece + 2 * LANES - 2) // LANES
    slot_rows = (slot_rows + SUBLANES - 1) // SUBLANES * SUBLANES
    depth = (count_len, columns, 1, LANES)
    minima = (count_len, n, SUBLANES, LANES)
    dma = pltpu.SemaphoreType.DMA

    groups = pl.pallas_call(
        functools.partial(
            profile_kernel, piece, n, count_len, len_devices, tile_list.shape[0]
        ),
        out_shape=jax.ShapeDtypeStruct((len_devices, count_len, SUBLANES, LANES), jnp.float32),
        in_specs=[pl.BlockSpec(memory_space=HBM)] * 4,
        out_specs=pl.BlockSpec(memory_space=VMEM),
        scratch_shapes=[
            pltpu.VMEM((piece,), jnp.float32),
            pltpu.SMEM(tile_list.shape[::-1], jnp.int32),
            pltpu.SMEM(window_lengths.shape, jnp.int32),
            pltpu.SMEM(exclusion.shape, jnp.int32),
            pltpu.VMEM((slot_rows * LANES,), jnp.float32),
            pltpu.VMEM((slot_rows, LANES), jnp.float32),
            pltpu.VMEM((n, slot_rows, LANES), jnp.float32),
            pltpu.VMEM((columns, LANES), jnp.float32),
            pltpu.VMEM((columns, LANES, LANES), jnp.float32),
            pltpu.VMEM(depth, jnp.float32),
            pltpu.VMEM(depth, jnp.float32),
            pltpu.VMEM((count_len, MAX_LEN, LANES), jnp.bfloat16),
            pltpu.VMEM((2, MAX_LEN, TILE_SIDE), jnp.bfloat16),
            pltpu.VMEM((2, MAX_LEN, TILE_SIDE), jnp.bfloat16),
            pltpu.VMEM(minima, jnp.float32),
            pltpu.VMEM(minima, jnp.float32),
            pltpu.VMEM((count_len, SUBLANES, LANES), jnp.float32),
            dma((4,)),
            dma((n,)),
            dma((n,)),
            dma((count_len, n)),
            dma((count_len, n)),
            dma((len_devices,)),
            dma((len_devices,)),
        ],
        compiler_params=pltpu.CompilerParams(
            collective_id=0,
            has_side_effects=True,
            vmem_limit_bytes=16 * GRANT + points * LANES * 4,
        ),
        name="profile",
    )(series, tile_list.T, window_lengths, exclusion)

    profile = jax.ShapeDtypeStruct((len_devices * count_len, TILE_SIDE), jnp.float32)
    return pl.pallas_call(
        write_kernel,
        out_shape=(profile, profile),
        in_specs=[pl.BlockSpec(memory_space=VMEM)],
        out_specs=(pl.BlockSpec(memory_space=HBM), pl.BlockSpec(memory_space=HBM)),
        scratch_shapes=[
            pltpu.VMEM(profile.shape, jnp.float32),
            pltpu.VMEM(profile.shape, jnp.float32),
            dma((2,)),
        ],
        name="write_profiles",
    )(groups)


def solution(mesh):
    return jax.shard_map(
        shards,
        mesh=mesh,
        in_specs=(P("tile"), P("len"), P("len"), P("tile", None)),
        out_specs=(P(None, "tile"), P(None, "tile")),
        check_vma=False,
    )
```

```python
import functools

import jax
import jax.numpy as jnp
from jax import lax
from jax.experimental import pallas as pl
from jax.experimental.pallas import tpu as pltpu
from jax.sharding import PartitionSpec as P

MAX_LEN = 1024
TILE_SIDE = 512
LANES = 128
SUBLANES = 8
GRANT = 1 << 20
QUARTERS = TILE_SIDE // LANES

VAR_EPS = 1e-05

VMEM = pltpu.MemorySpace.VMEM
SMEM = pltpu.MemorySpace.SMEM
HBM = pltpu.MemorySpace.HBM


def partner(me, step, n):
    if n & (n - 1):
        return lax.rem(me + step, n)
    peer = me
    for b in range(n.bit_length() - 1):
        if step >> b & 1:
            peer = peer + (1 << b) * (1 - 2 * lax.rem(lax.div(me, 1 << b), 2))
    return peer


def steps_of(n):
    return range(n - 1, 0, -1)


def signal_all(barrier, axis, n):
    me = lax.axis_index(axis)
    for step in range(1, n) if n & (n - 1) else steps_of(n):
        pl.semaphore_signal(
            barrier,
            inc=1,
            device_id={axis: partner(me, step, n)},
            device_id_type=pl.DeviceIdType.MESH,
        )


def copy_to(axis, n, step, source, target, send_sem, recv_sem):
    return pltpu.make_async_remote_copy(
        src_ref=source,
        dst_ref=target,
        send_sem=send_sem,
        recv_sem=recv_sem,
        device_id={axis: partner(lax.axis_index(axis), step, n)},
        device_id_type=pl.DeviceIdType.MESH,
    )


def shifted(values, count):
    rows = values.shape[0]
    skip, shift = count // LANES, count % LANES
    if shift:
        lane_ids = lax.broadcasted_iota(jnp.int32, values.shape, 1)
        values = pltpu.roll(values, LANES - shift, 1)
        values = jnp.where(lane_ids < LANES - shift, values, pltpu.roll(values, rows - 1, 0))
    if skip:
        values = pltpu.roll(values, rows - skip, 0)
    return values


def window_stats(packed, lengths):
    mean, spread = packed, jnp.zeros_like(packed)
    results = [(jnp.zeros_like(packed), jnp.zeros_like(packed)) for _ in lengths]
    bits = MAX_LEN.bit_length()
    for b in range(bits):
        first = 1 << b
        for l, length in enumerate(lengths):
            tail_mean, tail_spread = results[l]
            if b:
                tail_mean, tail_spread = shifted(tail_mean, first), shifted(tail_spread, first)
            rest = lax.rem(length, first).astype(jnp.float32)
            share = rest / (rest + first)
            gap = tail_mean - mean
            taken = (jnp.full(packed.shape, length) & first) != 0
            results[l] = (
                jnp.where(taken, mean + gap * share, results[l][0]),
                jnp.where(
                    taken, spread + tail_spread + gap * gap * (share * first), results[l][1]
                ),
            )
        if b < bits - 1:
            next_mean = shifted(mean, first)
            gap = next_mean - mean
            mean = 0.5 * (mean + next_mean)
            if b:
                spread = spread + shifted(spread, first) + gap * gap * (0.5 * first)
            else:
                spread = gap * gap * 0.5
    return [
        (mean, 1.0 / jnp.sqrt(spread / length.astype(jnp.float32) + VAR_EPS))
        for (mean, spread), length in zip(results, lengths)
    ]


def profile_kernel(
    piece,
    n,
    count_len,
    len_devices,
    slots_of_tiles,
    series_ref,
    tile_hbm,
    length_hbm,
    barrier_hbm,
    groups,
    piece_ref,
    tile_ref,
    length_ref,
    barrier_ref,
    flat,
    staged,
    slots,
    packed,
    base,
    centre_ref,
    inverse_ref,
    keep_ref,
    left_op,
    right_op,
    best,
    parts,
    mine,
    in_sem,
    send_piece,
    recv_piece,
    send_sem,
    recv_sem,
    send_len,
    recv_len,
):
    me = lax.axis_index("tile")
    my_len = lax.axis_index("len")
    loads = [
        pltpu.make_async_copy(source, target, in_sem.at[k])
        for k, (source, target) in enumerate(
            (
                (series_ref, piece_ref),
                (tile_hbm, tile_ref),
                (length_hbm, length_ref),
                (barrier_hbm, barrier_ref),
            )
        )
    ]
    loads[0].start()
    barrier = pltpu.get_barrier_semaphore()
    signal_all(barrier, "tile", n)
    signal_all(barrier, "len", len_devices)
    for load in loads[1:]:
        load.start()

    slot_rows = staged.shape[0]
    flat[...] = jnp.zeros(flat.shape, jnp.float32)
    loads[0].wait()
    flat[:piece] = piece_ref[...]
    values = flat[...].reshape(slot_rows, LANES)
    shift = lax.rem(me * piece, LANES)
    lane_ids = lax.broadcasted_iota(jnp.int32, values.shape, 1)
    values = pltpu.roll(values, shift, 1)
    staged[...] = jnp.where(lane_ids >= shift, values, pltpu.roll(values, 1, 0))

    pl.semaphore_wait(barrier, n - 1 + len_devices - 1)
    copies = [
        copy_to("tile", n, step, staged, slots.at[me], send_piece.at[step], recv_piece.at[step])
        for step in steps_of(n)
    ]
    for copy in copies:
        copy.start()
    slots[me] = staged[...]
    for load in loads[1:]:
        load.wait()

    lengths = [length_ref[l] for l in range(count_len)]
    row_ids = lax.broadcasted_iota(jnp.int32, (MAX_LEN, 2 * LANES), 0)
    row_ids = row_ids + (SUBLANES - 1) - 2 * lax.rem(row_ids, SUBLANES)
    for l, length in enumerate(lengths):
        keep_ref[l] = jnp.where(row_ids < length, 1.0, 0.0).astype(jnp.bfloat16)
        best[l] = jnp.full(best.shape[1:], -length.astype(jnp.float32), jnp.float32)
    packed[...] = jnp.zeros(packed.shape, jnp.float32)
    for copy in copies:
        copy.wait_recv()

    columns = packed.shape[0]
    for t in range(n):
        low, first = divmod(t * piece, LANES)
        used = (first + piece + LANES - 1) // LANES
        packed[low : low + used, :] += slots[t, :used, :]

    for l, (centre, inverse) in enumerate(window_stats(packed[...], lengths)):
        centre_ref[l] = centre.reshape(columns, 1, LANES)
        inverse_ref[l] = inverse.reshape(columns, 1, LANES)

    sub = lax.broadcasted_iota(jnp.int32, (SUBLANES, LANES), 0)
    lane = lax.broadcasted_iota(jnp.int32, (SUBLANES, LANES), 1)
    groups8 = LANES // SUBLANES
    span = 12 if columns % 12 == 0 else 1

    def spread_columns(k, turned):
        for j in range(span):
            a = columns - 1 - k * span - j
            row = jnp.broadcast_to(packed[pl.ds(a, 1), :], (SUBLANES, LANES))
            later = []
            for g in range(groups8):
                moved = pltpu.roll(row, LANES + 1 - SUBLANES * (g + 1), 1, stride=1, stride_axis=0)
                base[a, SUBLANES * g : SUBLANES * (g + 1), :] = jnp.where(
                    lane - sub < LANES + 1 - SUBLANES * (g + 1), moved, turned[g]
                )
                later.append(moved)
            turned = tuple(later)
        return turned

    lax.fori_loop(
        0,
        columns // span,
        spread_columns,
        (jnp.zeros((SUBLANES, LANES), jnp.float32),) * groups8,
    )

    def build(l, slot, buffer):
        firsts = [tile_ref[k, slot] * QUARTERS for k in range(2)]
        for k, (first, target) in enumerate(zip(firsts, (left_op, right_op))):
            centre, inverse = (
                jnp.concatenate([source[l, first + u] for u in range(QUARTERS)], axis=1)
                for source in (centre_ref, inverse_ref)
            )
            for c in range(MAX_LEN // LANES):
                rows = slice(c * LANES, (c + 1) * LANES)
                values = jnp.concatenate([base[first + u + c] for u in range(QUARTERS)], axis=1)
                normal = ((values - centre) * inverse).astype(jnp.bfloat16)
                if k == 0:
                    normal = normal * jnp.concatenate([keep_ref[l, rows, :]] * 2, axis=1)
                target[buffer, rows, :] = normal

    def product(l, slot, buffer):
        row_block, col_block = tile_ref[0, slot], tile_ref[1, slot]
        size = lengths[l].astype(jnp.float32)
        limit = barrier_ref[l] - (col_block - row_block) * TILE_SIDE
        tops = [None] * QUARTERS
        found = []
        for low in range(0, TILE_SIDE, 2 * LANES):
            values = lax.dot_general(
                left_op[buffer, :, low : low + 2 * LANES],
                right_op[buffer],
                (((0,), (0,)), ((), ())),
                preferred_element_type=jnp.float32,
            )
            ahead = lax.broadcasted_iota(jnp.int32, values.shape, 1) - (
                lax.broadcasted_iota(jnp.int32, values.shape, 0) + low
            )
            values = jnp.where(ahead > limit, values, -size)
            folded = None
            for u in range(QUARTERS):
                part = values[:, u * LANES : (u + 1) * LANES]
                folded = part if folded is None else jnp.maximum(folded, part)
                top = jnp.max(part, axis=0, keepdims=True)
                tops[u] = top if tops[u] is None else jnp.maximum(tops[u], top)
            for q in range(2):
                turned_back = jnp.transpose(folded[q * LANES : (q + 1) * LANES, :])
                found.append(jnp.max(turned_back, axis=0, keepdims=True))
        both = jnp.full((SUBLANES, LANES), -size, jnp.float32)
        for u in range(QUARTERS):
            both = jnp.where(sub == u, found[u], both)
            both = jnp.where(sub == QUARTERS + u, tops[u], both)
        row_is, col_is = jnp.full(sub.shape, row_block), jnp.full(sub.shape, col_block)
        owner = jnp.where(sub < QUARTERS, row_is, col_is)
        for b in range(n):
            old = best[l, b]
            best[l, b] = jnp.where(owner == b, jnp.maximum(old, both), old)

    sends = []
    work = [(l, slot) for l in range(count_len) for slot in range(slots_of_tiles)]
    build(*work[0], 0)
    for p, (l, slot) in enumerate(work):
        if p + 1 < len(work):
            build(*work[p + 1], (p + 1) % 2)
        product(l, slot, p % 2)
        if slot == slots_of_tiles - 1:
            sends.append(
                [
                    copy_to(
                        "tile",
                        n,
                        step,
                        best.at[l, partner(me, step, n)],
                        parts.at[l, step],
                        send_sem.at[l, step],
                        recv_sem.at[l, step],
                    )
                    for step in steps_of(n)
                ]
            )
            for copy in sends[-1]:
                copy.start()

    for l in range(count_len):
        for copy in sends[l]:
            copy.wait_recv()
        merged = best[l, me]
        for step in range(1, n):
            merged = jnp.maximum(merged, parts[l, step])
        merged = 1.0 - merged / lengths[l].astype(jnp.float32)
        mine[l] = merged
        groups[my_len, l] = merged
    copies_len = [
        copy_to("len", len_devices, step, mine, groups.at[my_len], send_len.at[step], recv_len.at[step])
        for step in range(1, len_devices)
    ]
    for copy in copies_len:
        copy.start()
    for copy in copies:
        copy.wait_send()
    for some in sends:
        for copy in some:
            copy.wait_send()
    for copy in copies_len:
        copy.wait()


def write_kernel(groups_ref, right_ref, left_ref, right, left, sems):
    len_devices, count_len = groups_ref.shape[:2]
    for g in range(len_devices):
        for l in range(count_len):
            row = g * count_len + l
            for u in range(QUARTERS):
                lanes = slice(u * LANES, (u + 1) * LANES)
                right[row : row + 1, lanes] = groups_ref[g, l, u : u + 1, :]
                left[row : row + 1, lanes] = groups_ref[g, l, QUARTERS + u : QUARTERS + u + 1, :]
    copies = [
        pltpu.make_async_copy(right, right_ref, sems.at[0]),
        pltpu.make_async_copy(left, left_ref, sems.at[1]),
    ]
    for copy in copies:
        copy.start()
    for copy in copies:
        copy.wait()


def shards(series, window_lengths, exclusion, tile_list):
    n = lax.axis_size("tile")
    len_devices = lax.axis_size("len")
    count_len = window_lengths.shape[0]
    piece = series.shape[0]
    points = piece * n
    columns = points // LANES
    blocks = (points - MAX_LEN) // TILE_SIDE
    assert blocks == n
    slot_rows = (piece + 2 * LANES - 2) // LANES
    slot_rows = (slot_rows + SUBLANES - 1) // SUBLANES * SUBLANES
    depth = (count_len, columns, 1, LANES)
    minima = (count_len, n, SUBLANES, LANES)
    dma = pltpu.SemaphoreType.DMA

    groups = pl.pallas_call(
        functools.partial(
            profile_kernel, piece, n, count_len, len_devices, tile_list.shape[0]
        ),
        out_shape=pltpu.VMEM((len_devices, count_len, SUBLANES, LANES), jnp.float32),
        in_specs=[pl.BlockSpec(memory_space=HBM)] * 4,
        out_specs=pl.BlockSpec(memory_space=VMEM),
        scratch_shapes=[
            pltpu.VMEM((piece,), jnp.float32),
            pltpu.SMEM(tile_list.shape[::-1], jnp.int32),
            pltpu.SMEM(window_lengths.shape, jnp.int32),
            pltpu.SMEM(exclusion.shape, jnp.int32),
            pltpu.VMEM((slot_rows * LANES,), jnp.float32),
            pltpu.VMEM((slot_rows, LANES), jnp.float32),
            pltpu.VMEM((n, slot_rows, LANES), jnp.float32),
            pltpu.VMEM((columns, LANES), jnp.float32),
            pltpu.VMEM((columns, LANES, LANES), jnp.float32),
            pltpu.VMEM(depth, jnp.float32),
            pltpu.VMEM(depth, jnp.float32),
            pltpu.VMEM((count_len, MAX_LEN, 2 * LANES), jnp.bfloat16),
            pltpu.VMEM((2, MAX_LEN, TILE_SIDE), jnp.bfloat16),
            pltpu.VMEM((2, MAX_LEN, TILE_SIDE), jnp.bfloat16),
            pltpu.VMEM(minima, jnp.float32),
            pltpu.VMEM(minima, jnp.float32),
            pltpu.VMEM((count_len, SUBLANES, LANES), jnp.float32),
            dma((4,)),
            dma((n,)),
            dma((n,)),
            dma((count_len, n)),
            dma((count_len, n)),
            dma((len_devices,)),
            dma((len_devices,)),
        ],
        compiler_params=pltpu.CompilerParams(
            collective_id=0,
            has_side_effects=True,
            vmem_limit_bytes=16 * GRANT + points * LANES * 4,
        ),
        name="profile",
    )(
        *(
            pltpu.with_memory_space_constraint(x, HBM)
            for x in (series, tile_list.T, window_lengths, exclusion)
        )
    )

    profile = jax.ShapeDtypeStruct((len_devices * count_len, TILE_SIDE), jnp.float32)
    return pl.pallas_call(
        write_kernel,
        out_shape=(profile, profile),
        in_specs=[pl.BlockSpec(memory_space=VMEM)],
        out_specs=(pl.BlockSpec(memory_space=HBM), pl.BlockSpec(memory_space=HBM)),
        scratch_shapes=[
            pltpu.VMEM(profile.shape, jnp.float32),
            pltpu.VMEM(profile.shape, jnp.float32),
            dma((2,)),
        ],
        compiler_params=pltpu.CompilerParams(vmem_limit_bytes=GRANT),
        name="write_profiles",
    )(groups)


def solution(mesh):
    return jax.shard_map(
        shards,
        mesh=mesh,
        in_specs=(P("tile"), P("len"), P("len"), P("tile", None)),
        out_specs=(P(None, "tile"), P(None, "tile")),
        check_vma=False,
    )
```

```python
import functools

import jax
import jax.numpy as jnp
from jax import lax
from jax.experimental import pallas as pl
from jax.experimental.pallas import tpu as pltpu
from jax.sharding import PartitionSpec as P

MAX_LEN = 1024
TILE_SIDE = 512
LANES = 128
SUBLANES = 8
GRANT = 1 << 20
QUARTERS = TILE_SIDE // LANES

EMPTY_VALUE = 2.0
VAR_EPS = 1e-05

VMEM = pltpu.MemorySpace.VMEM
SMEM = pltpu.MemorySpace.SMEM
HBM = pltpu.MemorySpace.HBM


def partner(me, step, n):
    peer = me
    for b in range(n.bit_length() - 1):
        if step >> b & 1:
            peer = peer + (1 << b) * (1 - 2 * lax.rem(lax.div(me, 1 << b), 2))
    return peer


def signal_all(barrier, axis, n):
    for step in range(n - 1, 0, -1):
        pl.semaphore_signal(
            barrier,
            inc=1,
            device_id={axis: partner(lax.axis_index(axis), step, n)},
            device_id_type=pl.DeviceIdType.MESH,
        )


def copy_to(source, target, send_sem, recv_sem, **peer):
    return pltpu.make_async_remote_copy(
        src_ref=source,
        dst_ref=target,
        send_sem=send_sem,
        recv_sem=recv_sem,
        device_id=peer,
        device_id_type=pl.DeviceIdType.MESH,
    )


def shifted(values, count):
    rows = values.shape[0]
    skip, shift = count // LANES, count % LANES
    if shift:
        lane_ids = lax.broadcasted_iota(jnp.int32, values.shape, 1)
        values = pltpu.roll(values, LANES - shift, 1)
        values = jnp.where(lane_ids < LANES - shift, values, pltpu.roll(values, rows - 1, 0))
    if skip:
        values = pltpu.roll(values, rows - skip, 0)
    return values


def window_stats(packed, lengths):
    mean, spread = packed, jnp.zeros_like(packed)
    results = [(jnp.zeros_like(packed), jnp.zeros_like(packed)) for _ in lengths]
    bits = MAX_LEN.bit_length()
    for b in range(bits):
        first = 1 << b
        for l, length in enumerate(lengths):
            tail_mean, tail_spread = results[l]
            if b:
                tail_mean, tail_spread = shifted(tail_mean, first), shifted(tail_spread, first)
            rest = lax.rem(length, first).astype(jnp.float32)
            share = rest / (rest + first)
            gap = tail_mean - mean
            taken = (jnp.full(packed.shape, length) & first) != 0
            results[l] = (
                jnp.where(taken, mean + gap * share, results[l][0]),
                jnp.where(
                    taken, spread + tail_spread + gap * gap * (share * first), results[l][1]
                ),
            )
        if b < bits - 1:
            next_mean = shifted(mean, first)
            gap = next_mean - mean
            mean = 0.5 * (mean + next_mean)
            if b:
                spread = spread + shifted(spread, first) + gap * gap * (0.5 * first)
            else:
                spread = gap * gap * 0.5
    return [
        (mean, 1.0 / jnp.sqrt(spread / length.astype(jnp.float32) + VAR_EPS))
        for (mean, spread), length in zip(results, lengths)
    ]


def profile_kernel(
    piece,
    n,
    count_len,
    len_devices,
    planes,
    chunk,
    slots_of_tiles,
    series_ref,
    tile_hbm,
    length_hbm,
    barrier_hbm,
    groups,
    piece_ref,
    tile_ref,
    length_ref,
    barrier_ref,
    flat,
    staged,
    slots,
    chunk_rows,
    packed,
    base,
    centre_ref,
    inverse_ref,
    keep_ref,
    left_op,
    right_op,
    best,
    parts,
    mine,
    in_sem,
    send_piece,
    recv_piece,
    send_sem,
    recv_sem,
    send_len,
    recv_len,
):
    me = lax.axis_index("tile")
    my_len = lax.axis_index("len")
    my_plane = my_len if planes > 1 else 0
    loads = [
        pltpu.make_async_copy(source, target, in_sem.at[k])
        for k, (source, target) in enumerate(
            (
                (series_ref, piece_ref),
                (tile_hbm, tile_ref),
                (length_hbm, length_ref),
                (barrier_hbm, barrier_ref),
            )
        )
    ]
    loads[0].start()
    barrier = pltpu.get_barrier_semaphore()
    for step in range(planes * n - 1, 0, -1):
        pl.semaphore_signal(
            barrier,
            inc=1,
            device_id={
                "len": partner(my_len, step // n, len_devices),
                "tile": partner(me, step % n, n),
            },
            device_id_type=pl.DeviceIdType.MESH,
        )
    greeted = planes * n - 1
    if planes == 1:
        signal_all(barrier, "len", len_devices)
        greeted += len_devices - 1
    for load in loads[1:]:
        load.start()

    slot_rows = staged.shape[0]
    flat[...] = jnp.zeros(flat.shape, jnp.float32)
    loads[0].wait()
    flat[:piece] = piece_ref[...]
    values = flat[...].reshape(slot_rows, LANES)
    shift = lax.rem(me * piece, LANES)
    lane_ids = lax.broadcasted_iota(jnp.int32, values.shape, 1)
    values = pltpu.roll(values, shift, 1)
    staged[...] = jnp.where(lane_ids >= shift, values, pltpu.roll(values, 1, 0))

    pl.semaphore_wait(barrier, greeted)
    copies = {
        step: copy_to(
            staged,
            slots.at[me],
            send_piece.at[step],
            recv_piece.at[step],
            tile=partner(me, step, n),
        )
        for step in range(n - 1, 0, -1)
    }
    for copy in copies.values():
        copy.start()
    slots[me] = staged[...]
    for load in loads[1:]:
        load.wait()

    lengths = [length_ref[l] for l in range(count_len)]
    row_ids = lax.broadcasted_iota(jnp.int32, (MAX_LEN, 2 * LANES), 0)
    row_ids = row_ids + (SUBLANES - 1) - 2 * lax.rem(row_ids, SUBLANES)
    for l, length in enumerate(lengths):
        keep_ref[l] = jnp.where(row_ids < length, 1.0, 0.0).astype(jnp.bfloat16)
    best[...] = jnp.full(best.shape, EMPTY_VALUE, jnp.float32)

    sub = lax.broadcasted_iota(jnp.int32, (SUBLANES, LANES), 0)
    lane = lax.broadcasted_iota(jnp.int32, (SUBLANES, LANES), 1)
    spans = [
        (
            LANES + 1 - SUBLANES * (g + 1),
            slice(SUBLANES * g, SUBLANES * (g + 1)),
            lane - sub < LANES + 1 - SUBLANES * (g + 1),
        )
        for g in range(LANES // SUBLANES)
    ]
    per = chunk * piece // LANES
    chunks = n // chunk

    def turn(row):
        row = jnp.broadcast_to(row, (SUBLANES, LANES))
        return [pltpu.roll(row, amount, 1, stride=1, stride_axis=0) for amount, _, _ in spans]

    for k in range(chunks):
        q = partner(lax.div(me, chunk), k, chunks)
        for step in range(k * chunk, (k + 1) * chunk):
            if step:
                copies[step].wait_recv()
        chunk_rows[q] = jnp.zeros(chunk_rows.shape[1:], jnp.float32)
        for t in range(chunk):
            low, first = divmod(t * piece, LANES)
            used = (first + piece + LANES - 1) // LANES
            chunk_rows[q, low : low + used, :] += slots[q * chunk + t, :used, :]
        later = None
        for j in range(per - 1, -1, -1):
            moved = turn(chunk_rows[q, j : j + 1, :])
            column = q * per + j + 1
            for g, (_, rows, here) in enumerate(spans):
                beyond = base[column, rows, :] if later is None else later[g]
                base[column, rows, :] = jnp.where(here, moved[g], beyond)
            later = moved
        for g, (_, rows, here) in enumerate(spans):
            base[q * per, rows, :] = jnp.where(here, base[q * per, rows, :], later[g])

    for q in range(chunks):
        packed[q * per : (q + 1) * per, :] = chunk_rows[q, :per, :]
    columns = packed.shape[0]
    for l, (centre, inverse) in enumerate(window_stats(packed[...], lengths)):
        centre_ref[l] = centre.reshape(columns, 1, LANES)
        inverse_ref[l] = inverse.reshape(columns, 1, LANES)

    def build(l, slot, buffer):
        firsts = [tile_ref[k, slot] * QUARTERS for k in range(2)]
        for k, (first, target) in enumerate(zip(firsts, (left_op, right_op))):
            centre, inverse = (
                jnp.concatenate([source[l, first + u] for u in range(QUARTERS)], axis=1)
                for source in (centre_ref, inverse_ref)
            )
            for c in range(MAX_LEN // LANES):
                rows = slice(c * LANES, (c + 1) * LANES)
                values = jnp.concatenate(
                    [base[first + u + c + 1] for u in range(QUARTERS)], axis=1
                )
                normal = ((values - centre) * inverse).astype(jnp.bfloat16)
                if k == 0:
                    normal = normal * jnp.concatenate([keep_ref[l, rows, :]] * 2, axis=1)
                target[buffer, rows, :] = normal

    def product(l, slot, buffer):
        row_block, col_block = tile_ref[0, slot], tile_ref[1, slot]
        size = lengths[l].astype(jnp.float32)
        limit = barrier_ref[l] - (col_block - row_block) * TILE_SIDE
        tops = [None] * QUARTERS
        found = []
        for low in range(0, TILE_SIDE, 2 * LANES):
            values = lax.dot_general(
                left_op[buffer, :, low : low + 2 * LANES],
                right_op[buffer],
                (((0,), (0,)), ((), ())),
                preferred_element_type=jnp.float32,
            )
            ahead = lax.broadcasted_iota(jnp.int32, values.shape, 1) - (
                lax.broadcasted_iota(jnp.int32, values.shape, 0) + low
            )
            values = jnp.where(ahead > limit, values, -size)
            folded = None
            for u in range(QUARTERS):
                part = values[:, u * LANES : (u + 1) * LANES]
                folded = part if folded is None else jnp.maximum(folded, part)
                top = jnp.max(part, axis=0, keepdims=True)
                tops[u] = top if tops[u] is None else jnp.maximum(tops[u], top)
            for q in range(2):
                turned_back = jnp.transpose(folded[q * LANES : (q + 1) * LANES, :])
                found.append(jnp.max(turned_back, axis=0, keepdims=True))
        both = jnp.broadcast_to(found[0], sub.shape)
        for u, row in enumerate([*found[1:], *tops]):
            both = jnp.where(sub == u + 1, row, both)
        both = 1.0 - both / size
        owner = jnp.where(
            sub < QUARTERS, jnp.full(sub.shape, row_block), jnp.full(sub.shape, col_block)
        )
        for b in range(n):
            old = best[l, b]
            best[l, b] = jnp.where(owner == b, jnp.minimum(old, both), old)

    def send(l):
        sent = [
            copy_to(
                best.at[l, partner(me, step % n, n)],
                parts.at[my_plane, l, step % n],
                send_sem.at[l, step],
                recv_sem.at[l, step],
                len=partner(my_len, step // n, len_devices),
                tile=partner(me, step % n, n),
            )
            for step in sorted(range(1, planes * n), key=lambda s: (s % n, s), reverse=True)
        ]
        for copy in sent:
            copy.start()
        return sent

    sends = []
    work = [(l, slot) for l in range(count_len) for slot in range(slots_of_tiles)]
    build(*work[0], 0)
    for p, (l, slot) in enumerate(work):
        if p + 1 < len(work):
            build(*work[p + 1], (p + 1) % 2)
        product(l, slot, p % 2)
        if slot == slots_of_tiles - 1:
            sends.append(send(l))
            parts[my_plane, l, 0] = best[l, me]

    for l in range(count_len):
        for copy in sends[l]:
            copy.wait_recv()
        for g in range(planes):
            merged = parts[g, l, 0]
            for step in range(1, n):
                merged = jnp.minimum(merged, parts[g, l, step])
            if planes > 1:
                groups[g, l] = merged
            else:
                mine[l] = merged
                groups[my_len, l] = merged
    if planes == 1:
        hops = [
            copy_to(
                mine,
                groups.at[my_len],
                send_len.at[step],
                recv_len.at[step],
                len=partner(my_len, step, len_devices),
            )
            for step in range(1, len_devices)
        ]
        for copy in hops:
            copy.start()
        for copy in hops:
            copy.wait()
    for copy in copies.values():
        copy.wait_send()
    for sent in sends:
        for copy in sent:
            copy.wait_send()


def write_kernel(groups_ref, right_ref, left_ref, right, left, sems):
    len_devices, count_len = groups_ref.shape[:2]
    for g in range(len_devices):
        for l in range(count_len):
            row = g * count_len + l
            for u in range(QUARTERS):
                lanes = slice(u * LANES, (u + 1) * LANES)
                right[row : row + 1, lanes] = groups_ref[g, l, u : u + 1, :]
                left[row : row + 1, lanes] = groups_ref[g, l, QUARTERS + u : QUARTERS + u + 1, :]
    copies = [
        pltpu.make_async_copy(right, right_ref, sems.at[0]),
        pltpu.make_async_copy(left, left_ref, sems.at[1]),
    ]
    for copy in copies:
        copy.start()
    for copy in copies:
        copy.wait()


def shards(series, window_lengths, exclusion, tile_list):
    n = lax.axis_size("tile")
    len_devices = lax.axis_size("len")
    count_len = window_lengths.shape[0]
    piece = series.shape[0]
    points = piece * n
    columns = points // LANES
    blocks = (points - MAX_LEN) // TILE_SIDE
    assert blocks == n
    slot_rows = (piece + 2 * LANES - 2) // LANES
    slot_rows = (slot_rows + SUBLANES - 1) // SUBLANES * SUBLANES
    depth = (count_len, columns, 1, LANES)
    chunk = next(g for g in range(1, n + 1) if n % g == 0 and g * piece % LANES == 0)
    per = chunk * piece // LANES
    chunk_rows = (per + SUBLANES - 1) // SUBLANES * SUBLANES
    planes = len_devices if len_devices <= 2 else 1
    minima = (count_len, n, SUBLANES, LANES)
    dma = pltpu.SemaphoreType.DMA

    groups = pl.pallas_call(
        functools.partial(
            profile_kernel,
            piece,
            n,
            count_len,
            len_devices,
            planes,
            chunk,
            tile_list.shape[0],
        ),
        out_shape=pltpu.VMEM((len_devices, count_len, SUBLANES, LANES), jnp.float32),
        in_specs=[pl.BlockSpec(memory_space=HBM)] * 4,
        out_specs=pl.BlockSpec(memory_space=VMEM),
        scratch_shapes=[
            pltpu.VMEM((piece,), jnp.float32),
            pltpu.SMEM(tile_list.shape[::-1], jnp.int32),
            pltpu.SMEM(window_lengths.shape, jnp.int32),
            pltpu.SMEM(exclusion.shape, jnp.int32),
            pltpu.VMEM((slot_rows * LANES,), jnp.float32),
            pltpu.VMEM((slot_rows, LANES), jnp.float32),
            pltpu.VMEM((n, slot_rows, LANES), jnp.float32),
            pltpu.VMEM((n // chunk, chunk_rows, LANES), jnp.float32),
            pltpu.VMEM((columns, LANES), jnp.float32),
            pltpu.VMEM((columns + 1, LANES, LANES), jnp.float32),
            pltpu.VMEM(depth, jnp.float32),
            pltpu.VMEM(depth, jnp.float32),
            pltpu.VMEM((count_len, MAX_LEN, 2 * LANES), jnp.bfloat16),
            pltpu.VMEM((2, MAX_LEN, TILE_SIDE), jnp.bfloat16),
            pltpu.VMEM((2, MAX_LEN, TILE_SIDE), jnp.bfloat16),
            pltpu.VMEM(minima, jnp.float32),
            pltpu.VMEM((planes, *minima), jnp.float32),
            pltpu.VMEM((count_len, SUBLANES, LANES), jnp.float32),
            dma((4,)),
            dma((n,)),
            dma((n,)),
            dma((count_len, planes * n)),
            dma((count_len, planes * n)),
            dma((len_devices,)),
            dma((len_devices,)),
        ],
        compiler_params=pltpu.CompilerParams(
            collective_id=0,
            has_side_effects=True,
            vmem_limit_bytes=16 * GRANT + points * LANES * 4,
        ),
        name="profile",
    )(
        *(
            pltpu.with_memory_space_constraint(x, HBM)
            for x in (series, tile_list.T, window_lengths, exclusion)
        )
    )

    profile = jax.ShapeDtypeStruct((len_devices * count_len, TILE_SIDE), jnp.float32)
    return pl.pallas_call(
        write_kernel,
        out_shape=(profile, profile),
        in_specs=[pl.BlockSpec(memory_space=VMEM)],
        out_specs=(pl.BlockSpec(memory_space=HBM), pl.BlockSpec(memory_space=HBM)),
        scratch_shapes=[
            pltpu.VMEM(profile.shape, jnp.float32),
            pltpu.VMEM(profile.shape, jnp.float32),
            dma((2,)),
        ],
        compiler_params=pltpu.CompilerParams(vmem_limit_bytes=GRANT),
        name="write_profiles",
    )(groups)


def solution(mesh):
    return jax.shard_map(
        shards,
        mesh=mesh,
        in_specs=(P("tile"), P("len"), P("len"), P("tile", None)),
        out_specs=(P(None, "tile"), P(None, "tile")),
        check_vma=False,
    )
```

```python
import functools

import jax
import jax.numpy as jnp
from jax import lax
from jax.experimental import pallas as pl
from jax.experimental.pallas import tpu as pltpu
from jax.sharding import PartitionSpec as P

MAX_LEN = 1024
TILE_SIDE = 512
LANES = 128
SUBLANES = 8
GRANT = 1 << 20
QUARTERS = TILE_SIDE // LANES

EMPTY_VALUE = 2.0
VAR_EPS = 1e-05

VMEM = pltpu.MemorySpace.VMEM
SMEM = pltpu.MemorySpace.SMEM
HBM = pltpu.MemorySpace.HBM


def partner(me, step, n):
    peer = me
    for b in range(n.bit_length() - 1):
        if step >> b & 1:
            peer = peer + (1 << b) * (1 - 2 * lax.rem(lax.div(me, 1 << b), 2))
    return peer


def signal_all(barrier, axis, n):
    for step in range(n - 1, 0, -1):
        pl.semaphore_signal(
            barrier,
            inc=1,
            device_id={axis: partner(lax.axis_index(axis), step, n)},
            device_id_type=pl.DeviceIdType.MESH,
        )


def copy_to(source, target, send_sem, recv_sem, **peer):
    return pltpu.make_async_remote_copy(
        src_ref=source,
        dst_ref=target,
        send_sem=send_sem,
        recv_sem=recv_sem,
        device_id=peer,
        device_id_type=pl.DeviceIdType.MESH,
    )


def shifted(values, count):
    rows = values.shape[0]
    skip, shift = count // LANES, count % LANES
    if shift:
        lane_ids = lax.broadcasted_iota(jnp.int32, values.shape, 1)
        values = pltpu.roll(values, LANES - shift, 1)
        values = jnp.where(lane_ids < LANES - shift, values, pltpu.roll(values, rows - 1, 0))
    if skip:
        values = pltpu.roll(values, rows - skip, 0)
    return values


def window_stats(packed, lengths):
    mean, spread = packed, jnp.zeros_like(packed)
    results = [(jnp.zeros_like(packed), jnp.zeros_like(packed)) for _ in lengths]
    bits = MAX_LEN.bit_length()
    for b in range(bits):
        first = 1 << b
        for l, length in enumerate(lengths):
            tail_mean, tail_spread = results[l]
            if b:
                tail_mean, tail_spread = shifted(tail_mean, first), shifted(tail_spread, first)
            rest = lax.rem(length, first).astype(jnp.float32)
            share = rest / (rest + first)
            gap = tail_mean - mean
            taken = (jnp.full(packed.shape, length) & first) != 0
            results[l] = (
                jnp.where(taken, mean + gap * share, results[l][0]),
                jnp.where(
                    taken, spread + tail_spread + gap * gap * (share * first), results[l][1]
                ),
            )
        if b < bits - 1:
            next_mean = shifted(mean, first)
            gap = next_mean - mean
            mean = 0.5 * (mean + next_mean)
            if b:
                spread = spread + shifted(spread, first) + gap * gap * (0.5 * first)
            else:
                spread = gap * gap * 0.5
    return [
        (mean, 1.0 / jnp.sqrt(spread / length.astype(jnp.float32) + VAR_EPS))
        for (mean, spread), length in zip(results, lengths)
    ]


def profile_kernel(
    piece,
    n,
    count_len,
    len_devices,
    planes,
    chunk,
    deferred,
    series_ref,
    tile_hbm,
    length_hbm,
    barrier_hbm,
    groups,
    piece_ref,
    tile_ref,
    tile_in,
    length_ref,
    barrier_ref,
    flat,
    staged,
    slots,
    chunk_rows,
    packed,
    base,
    centre_ref,
    inverse_ref,
    keep_ref,
    left_op,
    right_op,
    best,
    parts,
    mine,
    in_sem,
    tile_sem,
    send_tile,
    recv_tile,
    send_piece,
    recv_piece,
    send_sem,
    recv_sem,
    send_len,
    recv_len,
):
    me = lax.axis_index("tile")
    my_len = lax.axis_index("len")
    my_plane = my_len if planes > 1 else 0
    loads = [
        pltpu.make_async_copy(source, target, in_sem.at[k])
        for k, (source, target) in enumerate(
            (
                (series_ref, piece_ref),
                (tile_hbm, tile_ref.at[0]),
                (length_hbm, length_ref),
                (barrier_hbm, barrier_ref),
            )
        )
    ]
    loads[0].start()
    barrier = pltpu.get_barrier_semaphore()
    for step in range(planes * n - 1, 0, -1):
        pl.semaphore_signal(
            barrier,
            inc=1,
            device_id={
                "len": partner(my_len, step // n, len_devices),
                "tile": partner(me, step % n, n),
            },
            device_id_type=pl.DeviceIdType.MESH,
        )
    greeted = planes * n - 1
    if planes == 1:
        signal_all(barrier, "len", len_devices)
        greeted += len_devices - 1
    for load in loads[1:]:
        load.start()

    slot_rows = staged.shape[0]
    flat[...] = jnp.zeros(flat.shape, jnp.float32)
    loads[0].wait()
    flat[:piece] = piece_ref[...]
    values = flat[...].reshape(slot_rows, LANES)
    shift = lax.rem(me * piece, LANES)
    lane_ids = lax.broadcasted_iota(jnp.int32, values.shape, 1)
    values = pltpu.roll(values, shift, 1)
    staged[...] = jnp.where(lane_ids >= shift, values, pltpu.roll(values, 1, 0))

    pl.semaphore_wait(barrier, greeted)
    copies = {
        step: copy_to(
            staged,
            slots.at[me],
            send_piece.at[step],
            recv_piece.at[step],
            tile=partner(me, step, n),
        )
        for step in range(n - 1, 0, -1)
    }
    for copy in copies.values():
        copy.start()
    share = count_len
    passed = [
        copy_to(
            tile_hbm,
            tile_in.at[e],
            send_tile.at[e],
            recv_tile.at[e],
            tile=partner(me, e, n),
        )
        for e in range(1, share)
    ]
    for copy in passed:
        copy.start()
    slots[me] = staged[...]
    for load in loads[1:]:
        load.wait()

    turn_of_mine = lax.rem(me, share)
    length, excluded = length_ref[turn_of_mine], barrier_ref[turn_of_mine]
    size = length.astype(jnp.float32)
    row_ids = lax.broadcasted_iota(jnp.int32, (MAX_LEN, 2 * LANES), 0)
    row_ids = row_ids + (SUBLANES - 1) - 2 * lax.rem(row_ids, SUBLANES)
    keep_ref[...] = jnp.where(row_ids < length, 1.0, 0.0).astype(jnp.bfloat16)
    for ref in best:
        ref[...] = jnp.full(ref.shape, EMPTY_VALUE, jnp.float32)

    sub = lax.broadcasted_iota(jnp.int32, (SUBLANES, LANES), 0)
    lane = lax.broadcasted_iota(jnp.int32, (SUBLANES, LANES), 1)
    spans = [
        (
            LANES + 1 - SUBLANES * (g + 1),
            slice(SUBLANES * g, SUBLANES * (g + 1)),
            lane - sub < LANES + 1 - SUBLANES * (g + 1),
        )
        for g in range(LANES // SUBLANES)
    ]
    per = chunk * piece // LANES
    chunks = n // chunk

    def turn(row):
        row = jnp.broadcast_to(row, (SUBLANES, LANES))
        return [pltpu.roll(row, amount, 1, stride=1, stride_axis=0) for amount, _, _ in spans]

    for k in range(chunks):
        q = partner(lax.div(me, chunk), k, chunks)
        for step in range(k * chunk, (k + 1) * chunk):
            if step:
                copies[step].wait_recv()
        chunk_rows[q] = jnp.zeros(chunk_rows.shape[1:], jnp.float32)
        for t in range(chunk):
            low, first = divmod(t * piece, LANES)
            used = (first + piece + LANES - 1) // LANES
            chunk_rows[q, low : low + used, :] += slots[q * chunk + t, :used, :]
        later = None
        for j in range(per - 1, -1, -1):
            moved = turn(chunk_rows[q, j : j + 1, :])
            column = q * per + j + 1
            for g, (_, rows, here) in enumerate(spans):
                beyond = base[column, rows, :] if later is None else later[g]
                base[column, rows, :] = jnp.where(here, moved[g], beyond)
            later = moved
        for g, (_, rows, here) in enumerate(spans):
            base[q * per, rows, :] = jnp.where(here, base[q * per, rows, :], later[g])

    for copy in passed:
        copy.wait_recv()
    moves = [
        pltpu.make_async_copy(tile_in.at[e], tile_ref.at[e], tile_sem.at[e]) for e in range(1, share)
    ]
    for move in moves:
        move.start()
    for q in range(chunks):
        packed[q * per : (q + 1) * per, :] = chunk_rows[q, :per, :]
    columns = packed.shape[0]
    ((centre, inverse),) = window_stats(packed[...], [length])
    centre_ref[...] = centre.reshape(columns, 1, LANES)
    inverse_ref[...] = inverse.reshape(columns, 1, LANES)
    for move in moves:
        move.wait()

    tiles = [(e, slot) for e in range(share) for slot in range(tile_ref.shape[2])]
    blocks_of = [[tile_ref[e, k, slot] for k in range(2)] for e, slot in tiles]
    half = TILE_SIDE // 2

    def build(t):
        for k, target in enumerate((left_op, right_op)):
            first = blocks_of[t][k] * QUARTERS
            centre, inverse = (
                jnp.concatenate([source[first + u] for u in range(QUARTERS)], axis=1)
                for source in (centre_ref, inverse_ref)
            )
            for c in range(MAX_LEN // LANES):
                rows = slice(c * LANES, (c + 1) * LANES)
                values = jnp.concatenate(
                    [base[first + u + c + 1] for u in range(QUARTERS)], axis=1
                )
                normal = ((values - centre) * inverse).astype(jnp.bfloat16)
                if k == 0:
                    normal = normal * jnp.concatenate([keep_ref[rows, :]] * 2, axis=1)
                target[t, rows, :] = normal

    def product(t, row, col, width):
        row_block, col_block = blocks_of[t]
        limit = excluded - (col_block - row_block) * TILE_SIDE
        values = lax.dot_general(
            left_op[t, :, row : row + half],
            right_op[t, :, col : col + width],
            (((0,), (0,)), ((), ())),
            preferred_element_type=jnp.float32,
        )
        ahead = (lax.broadcasted_iota(jnp.int32, values.shape, 1) + col) - (
            lax.broadcasted_iota(jnp.int32, values.shape, 0) + row
        )
        values = jnp.where(ahead > limit, values, -size)
        folded, tops = None, []
        for u in range(0, width, LANES):
            part = values[:, u : u + LANES]
            folded = part if folded is None else jnp.maximum(folded, part)
            tops.append(jnp.max(part, axis=0, keepdims=True))
        found = [
            jnp.max(jnp.transpose(folded[u : u + LANES, :]), axis=0, keepdims=True)
            for u in range(0, half, LANES)
        ]
        return found, tops

    def larger(some, others):
        return [jnp.maximum(x, y) for x, y in zip(some, others)]

    def update(r, t, right, left):
        row_block, col_block = blocks_of[t]
        ref = best[r]
        lines = lax.broadcasted_iota(jnp.int32, ref.shape[1:], 0)
        found = jnp.broadcast_to((right + left)[0], ref.shape[1:])
        for u, line in enumerate((right + left)[1:]):
            found = jnp.where(lines == u + 1, line, found)
        found = 1.0 - found / size
        owner = jnp.where(
            lines < len(right), jnp.full(lines.shape, row_block), jnp.full(lines.shape, col_block)
        )
        for b in range(n):
            ref[b] = jnp.minimum(ref[b], jnp.where(owner == b, found, EMPTY_VALUE))

    def send(r):
        sent = [
            copy_to(
                best[r].at[partner(me, step % n, n)],
                parts[r].at[my_plane, step % n],
                send_sem.at[r, step],
                recv_sem.at[r, step],
                len=partner(my_len, step // n, len_devices),
                tile=partner(me, step % n, n),
            )
            for step in sorted(range(1, planes * n), key=lambda s: (s % n, s), reverse=True)
        ]
        for copy in sent:
            copy.start()
        parts[r][my_plane, 0] = best[r][me]
        return sent

    late = range(len(tiles) - deferred, len(tiles))
    tops_of, found_of = {}, {}
    build(0)
    for t in range(len(tiles)):
        if t + 1 < len(tiles):
            build(t + 1)
        found, tops_of[t] = product(t, 0, 0, TILE_SIDE)
        update(0, t, found, [])
        if t not in late:
            found, tops = product(t, half, 0, TILE_SIDE)
            tops = larger(tops, tops_of[t])
            update(1, t, [], tops[:2])
            update(2, t, found, tops[2:])
    sends = [send(0)]
    for t in late:
        found_of[t], tops = product(t, half, 0, half)
        update(1, t, [], larger(tops, tops_of[t][:2]))
    sends.append(send(1))
    for t in late:
        found, tops = product(t, half, half, half)
        update(2, t, larger(found, found_of[t]), larger(tops, tops_of[t][2:]))
    sends.append(send(2))

    filled = 0
    for r, ref in enumerate(parts):
        for copy in sends[r]:
            copy.wait_recv()
        lines = slice(filled, filled + ref.shape[2])
        filled += ref.shape[2]
        for g in range(planes):
            for e in range(share):
                merged = ref[g, e]
                for step in range(e + share, n, share):
                    merged = jnp.minimum(merged, ref[g, step])
                l = partner(turn_of_mine, e, share)
                if planes > 1:
                    groups[g, l, lines, :] = merged
                else:
                    mine[l, lines, :] = merged
                    groups[my_len, l, lines, :] = merged
    if planes == 1:
        hops = [
            copy_to(
                mine,
                groups.at[my_len],
                send_len.at[step],
                recv_len.at[step],
                len=partner(my_len, step, len_devices),
            )
            for step in range(1, len_devices)
        ]
        for copy in hops:
            copy.start()
        for copy in hops:
            copy.wait()
    for copy in [*copies.values(), *passed]:
        copy.wait_send()
    for sent in sends:
        for copy in sent:
            copy.wait_send()


def write_kernel(groups_ref, right_ref, left_ref, right, left, sems):
    len_devices, count_len = groups_ref.shape[:2]
    for g in range(len_devices):
        for l in range(count_len):
            row = g * count_len + l
            for u in range(QUARTERS):
                lanes = slice(u * LANES, (u + 1) * LANES)
                line = u + u // 2 * 2
                right[row : row + 1, lanes] = groups_ref[g, l, line : line + 1, :]
                left[row : row + 1, lanes] = groups_ref[g, l, line + 2 : line + 3, :]
    copies = [
        pltpu.make_async_copy(right, right_ref, sems.at[0]),
        pltpu.make_async_copy(left, left_ref, sems.at[1]),
    ]
    for copy in copies:
        copy.start()
    for copy in copies:
        copy.wait()


def shards(series, window_lengths, exclusion, tile_list):
    n = lax.axis_size("tile")
    len_devices = lax.axis_size("len")
    count_len = window_lengths.shape[0]
    piece = series.shape[0]
    points = piece * n
    columns = points // LANES
    blocks = (points - MAX_LEN) // TILE_SIDE
    assert blocks == n
    slot_rows = (piece + 2 * LANES - 2) // LANES
    slot_rows = (slot_rows + SUBLANES - 1) // SUBLANES * SUBLANES
    depth = (columns, 1, LANES)
    chunk = next(g for g in range(1, n + 1) if n % g == 0 and g * piece % LANES == 0)
    per = chunk * piece // LANES
    chunk_rows = (per + SUBLANES - 1) // SUBLANES * SUBLANES
    planes = len_devices if len_devices <= 2 else 1
    share = count_len
    assert n % share == 0 and share & (share - 1) == 0
    rounds = (2, 2, 4)
    dma = pltpu.SemaphoreType.DMA

    groups = pl.pallas_call(
        functools.partial(
            profile_kernel,
            piece,
            n,
            count_len,
            len_devices,
            planes,
            chunk,
            share * tile_list.shape[0] // 2,
        ),
        out_shape=pltpu.VMEM((len_devices, count_len, SUBLANES, LANES), jnp.float32),
        in_specs=[pl.BlockSpec(memory_space=HBM)] * 4,
        out_specs=pl.BlockSpec(memory_space=VMEM),
        scratch_shapes=[
            pltpu.VMEM((piece,), jnp.float32),
            pltpu.SMEM((share, *tile_list.shape[::-1]), jnp.int32),
            pltpu.VMEM((share, *tile_list.shape[::-1]), jnp.int32),
            pltpu.SMEM(window_lengths.shape, jnp.int32),
            pltpu.SMEM(exclusion.shape, jnp.int32),
            pltpu.VMEM((slot_rows * LANES,), jnp.float32),
            pltpu.VMEM((slot_rows, LANES), jnp.float32),
            pltpu.VMEM((n, slot_rows, LANES), jnp.float32),
            pltpu.VMEM((n // chunk, chunk_rows, LANES), jnp.float32),
            pltpu.VMEM((columns, LANES), jnp.float32),
            pltpu.VMEM((columns + 1, LANES, LANES), jnp.float32),
            pltpu.VMEM(depth, jnp.float32),
            pltpu.VMEM(depth, jnp.float32),
            pltpu.VMEM((MAX_LEN, 2 * LANES), jnp.bfloat16),
            pltpu.VMEM((share * tile_list.shape[0], MAX_LEN, TILE_SIDE), jnp.bfloat16),
            pltpu.VMEM((share * tile_list.shape[0], MAX_LEN, TILE_SIDE), jnp.bfloat16),
            tuple(pltpu.VMEM((n, lines, LANES), jnp.float32) for lines in rounds),
            tuple(pltpu.VMEM((planes, n, lines, LANES), jnp.float32) for lines in rounds),
            pltpu.VMEM((count_len, SUBLANES, LANES), jnp.float32),
            dma((4,)),
            dma((share,)),
            dma((share,)),
            dma((share,)),
            dma((n,)),
            dma((n,)),
            dma((len(rounds), planes * n)),
            dma((len(rounds), planes * n)),
            dma((len_devices,)),
            dma((len_devices,)),
        ],
        compiler_params=pltpu.CompilerParams(
            collective_id=0,
            has_side_effects=True,
            vmem_limit_bytes=28 * GRANT + points * LANES * 4,
        ),
        name="profile",
    )(
        *(
            pltpu.with_memory_space_constraint(x, HBM)
            for x in (series, tile_list.T, window_lengths, exclusion)
        )
    )

    profile = jax.ShapeDtypeStruct((len_devices * count_len, TILE_SIDE), jnp.float32)
    return pl.pallas_call(
        write_kernel,
        out_shape=(profile, profile),
        in_specs=[pl.BlockSpec(memory_space=VMEM)],
        out_specs=(pl.BlockSpec(memory_space=HBM), pl.BlockSpec(memory_space=HBM)),
        scratch_shapes=[
            pltpu.VMEM(profile.shape, jnp.float32),
            pltpu.VMEM(profile.shape, jnp.float32),
            dma((2,)),
        ],
        compiler_params=pltpu.CompilerParams(vmem_limit_bytes=GRANT),
        name="write_profiles",
    )(groups)


def solution(mesh):
    return jax.shard_map(
        shards,
        mesh=mesh,
        in_specs=(P("tile"), P("len"), P("len"), P("tile", None)),
        out_specs=(P(None, "tile"), P(None, "tile")),
        check_vma=False,
    )
```

```python
import functools

import jax
import jax.numpy as jnp
from jax import lax
from jax.experimental import pallas as pl
from jax.experimental.pallas import tpu as pltpu
from jax.sharding import PartitionSpec as P

MAX_LEN = 1024
TILE_SIDE = 512
LANES = 128
SUBLANES = 8
GRANT = 1 << 20
QUARTERS = TILE_SIDE // LANES

EMPTY_VALUE = 2.0
VAR_EPS = 1e-05

VMEM = pltpu.MemorySpace.VMEM
SMEM = pltpu.MemorySpace.SMEM
HBM = pltpu.MemorySpace.HBM


def partner(me, step, n):
    peer = me
    for b in range(n.bit_length() - 1):
        if step >> b & 1:
            peer = peer + (1 << b) * (1 - 2 * lax.rem(lax.div(me, 1 << b), 2))
    return peer


def signal_all(barrier, axis, n):
    for step in range(n - 1, 0, -1):
        pl.semaphore_signal(
            barrier,
            inc=1,
            device_id={axis: partner(lax.axis_index(axis), step, n)},
            device_id_type=pl.DeviceIdType.MESH,
        )


def await_all(ref, sem, sent):
    copy = copy_to(ref, ref, sem, sem)
    copy.wait_send() if sent else copy.wait_recv()


def copy_to(source, target, send_sem, recv_sem, **peer):
    return pltpu.make_async_remote_copy(
        src_ref=source,
        dst_ref=target,
        send_sem=send_sem,
        recv_sem=recv_sem,
        device_id=peer,
        device_id_type=pl.DeviceIdType.MESH,
    )


def shifted(values, count):
    rows = values.shape[0]
    skip, shift = count // LANES, count % LANES
    if shift:
        lane_ids = lax.broadcasted_iota(jnp.int32, values.shape, 1)
        values = pltpu.roll(values, LANES - shift, 1)
        values = jnp.where(lane_ids < LANES - shift, values, pltpu.roll(values, rows - 1, 0))
    if skip:
        values = pltpu.roll(values, rows - skip, 0)
    return values


def window_stats(packed, lengths):
    mean, spread = packed, jnp.zeros_like(packed)
    results = [(jnp.zeros_like(packed), jnp.zeros_like(packed)) for _ in lengths]
    bits = MAX_LEN.bit_length()
    for b in range(bits):
        first = 1 << b
        for l, length in enumerate(lengths):
            tail_mean, tail_spread = results[l]
            if b:
                tail_mean, tail_spread = shifted(tail_mean, first), shifted(tail_spread, first)
            rest = lax.rem(length, first).astype(jnp.float32)
            share = rest / (rest + first)
            gap = tail_mean - mean
            taken = (jnp.full(packed.shape, length) & first) != 0
            results[l] = (
                jnp.where(taken, mean + gap * share, results[l][0]),
                jnp.where(
                    taken, spread + tail_spread + gap * gap * (share * first), results[l][1]
                ),
            )
        if b < bits - 1:
            next_mean = shifted(mean, first)
            gap = next_mean - mean
            mean = 0.5 * (mean + next_mean)
            if b:
                spread = spread + shifted(spread, first) + gap * gap * (0.5 * first)
            else:
                spread = gap * gap * 0.5
    return [
        (mean, 1.0 / jnp.sqrt(spread / length.astype(jnp.float32) + VAR_EPS))
        for (mean, spread), length in zip(results, lengths)
    ]


def profile_kernel(
    piece,
    n,
    count_len,
    len_devices,
    planes,
    chunk,
    series_ref,
    tile_hbm,
    length_hbm,
    barrier_hbm,
    groups,
    piece_ref,
    tile_ref,
    length_ref,
    barrier_ref,
    flat,
    staged,
    slots,
    chunk_rows,
    packed,
    base,
    centre_ref,
    inverse_ref,
    keep_ref,
    left_op,
    right_op,
    best,
    parts,
    mine,
    in_sem,
    send_tile,
    recv_tile,
    plane_sem,
    send_piece,
    recv_piece,
    send_sem,
    recv_sem,
    send_len,
    recv_len,
):
    me = lax.axis_index("tile")
    my_len = lax.axis_index("len")
    my_plane = my_len if planes > 1 else 0
    loads = [
        pltpu.make_async_copy(source, target, in_sem.at[k])
        for k, (source, target) in enumerate(
            (
                (series_ref, piece_ref),
                (tile_hbm, tile_ref.at[0]),
                (length_hbm, length_ref),
                (barrier_hbm, barrier_ref),
            )
        )
    ]
    loads[0].start()
    barrier = pltpu.get_barrier_semaphore()
    signal_all(barrier, "tile", n)
    signal_all(barrier, "len", len_devices)
    for load in loads[1:]:
        load.start()

    slot_rows = staged.shape[0]
    flat[...] = jnp.zeros(flat.shape, jnp.float32)
    loads[0].wait()
    flat[:piece] = piece_ref[...]
    values = flat[...].reshape(slot_rows, LANES)
    shift = lax.rem(me * piece, LANES)
    lane_ids = lax.broadcasted_iota(jnp.int32, values.shape, 1)
    values = pltpu.roll(values, shift, 1)
    staged[...] = jnp.where(lane_ids >= shift, values, pltpu.roll(values, 1, 0))

    pl.semaphore_wait(barrier, n - 1 + len_devices - 1)
    for step in range(n - 1, 0, -1):
        copy_to(
            staged,
            slots.at[me],
            send_piece,
            recv_piece.at[step // chunk],
            tile=partner(me, step, n),
        ).start()
    if planes > 1:
        for step in range(1, len_devices):
            pl.semaphore_signal(
                plane_sem,
                inc=1,
                device_id={"len": partner(my_len, step, len_devices)},
                device_id_type=pl.DeviceIdType.MESH,
            )
    slots[me] = staged[...]
    for load in loads[1:]:
        load.wait()
    share = count_len
    passed = [
        copy_to(
            tile_ref.at[0],
            tile_ref.at[e],
            send_tile.at[e],
            recv_tile.at[e],
            tile=partner(me, e, n),
        )
        for e in range(1, share)
    ]
    for copy in passed:
        copy.start()

    turn_of_mine = lax.rem(me, share)
    length, excluded = length_ref[turn_of_mine], barrier_ref[turn_of_mine]
    size = length.astype(jnp.float32)
    row_ids = lax.broadcasted_iota(jnp.int32, (MAX_LEN, 2 * LANES), 0)
    row_ids = row_ids + (SUBLANES - 1) - 2 * lax.rem(row_ids, SUBLANES)
    keep_ref[...] = jnp.where(row_ids < length, 1.0, 0.0).astype(jnp.bfloat16)
    best[...] = jnp.full(best.shape, EMPTY_VALUE, jnp.float32)

    sub = lax.broadcasted_iota(jnp.int32, (SUBLANES, LANES), 0)
    lane = lax.broadcasted_iota(jnp.int32, (SUBLANES, LANES), 1)
    spans = [
        (
            LANES + 1 - SUBLANES * (g + 1),
            slice(SUBLANES * g, SUBLANES * (g + 1)),
            lane - sub < LANES + 1 - SUBLANES * (g + 1),
        )
        for g in range(LANES // SUBLANES)
    ]
    per = chunk * piece // LANES
    chunks = n // chunk

    def turn(row):
        row = jnp.broadcast_to(row, (SUBLANES, LANES))
        row = pltpu.roll(row, LANES + 1 - SUBLANES, 1, stride=1, stride_axis=0)
        return [row] + [pltpu.roll(row, LANES - SUBLANES * g, 1) for g in range(1, len(spans))]

    for k in range(chunks):
        q = partner(lax.div(me, chunk), k, chunks)
        coming = chunk if k else chunk - 1
        if coming:
            await_all(slots.at[pl.ds(0, coming)], recv_piece.at[k], False)
        chunk_rows[q] = jnp.zeros(chunk_rows.shape[1:], jnp.float32)
        for t in range(chunk):
            low, first = divmod(t * piece, LANES)
            used = (first + piece + LANES - 1) // LANES
            chunk_rows[q, low : low + used, :] += slots[q * chunk + t, :used, :]
        later = None
        for j in range(per - 1, -1, -1):
            moved = turn(chunk_rows[q, j : j + 1, :])
            column = q * per + j + 1
            for g, (_, rows, here) in enumerate(spans):
                beyond = base[column, rows, :] if later is None else later[g]
                base[column, rows, :] = jnp.where(here, moved[g], beyond)
            later = moved
        for g, (_, rows, here) in enumerate(spans):
            base[q * per, rows, :] = jnp.where(here, base[q * per, rows, :], later[g])

    for copy in passed:
        copy.wait()
    await_all(slots.at[pl.ds(0, n - 1)], send_piece, True)
    for q in range(chunks):
        packed[q * per : (q + 1) * per, :] = chunk_rows[q, :per, :]
    columns = packed.shape[0]
    ((centre, inverse),) = window_stats(packed[...], [length])
    centre_ref[...] = centre.reshape(columns, 1, LANES)
    inverse_ref[...] = inverse.reshape(columns, 1, LANES)

    tiles = [(e, slot) for e in range(share) for slot in range(tile_ref.shape[2])]
    blocks_of = [[tile_ref[e, k, slot] for k in range(2)] for e, slot in tiles]

    def build(t):
        for k, target in enumerate((left_op, right_op)):
            first = blocks_of[t][k] * QUARTERS
            centre, inverse = (
                jnp.concatenate([source[first + u] for u in range(QUARTERS)], axis=1)
                for source in (centre_ref, inverse_ref)
            )
            for c in range(MAX_LEN // LANES):
                rows = slice(c * LANES, (c + 1) * LANES)
                values = jnp.concatenate(
                    [base[first + u + c + 1] for u in range(QUARTERS)], axis=1
                )
                normal = ((values - centre) * inverse).astype(jnp.bfloat16)
                if k == 0:
                    normal = normal * jnp.concatenate([keep_ref[rows, :]] * 2, axis=1)
                target[t, rows, :] = normal

    def product(t):
        row_block, col_block = blocks_of[t]
        limit = excluded - (col_block - row_block) * TILE_SIDE
        tops, found = [None] * QUARTERS, []
        for low in range(0, TILE_SIDE, 2 * LANES):
            values = lax.dot_general(
                left_op[t, :, low : low + 2 * LANES],
                right_op[t],
                (((0,), (0,)), ((), ())),
                preferred_element_type=jnp.float32,
            )
            ahead = lax.broadcasted_iota(jnp.int32, values.shape, 1) - (
                lax.broadcasted_iota(jnp.int32, values.shape, 0) + low
            )
            values = jnp.where(ahead > limit, values, -size)
            folded = None
            for u in range(QUARTERS):
                part = values[:, u * LANES : (u + 1) * LANES]
                folded = part if folded is None else jnp.maximum(folded, part)
                top = jnp.max(part, axis=0, keepdims=True)
                tops[u] = top if tops[u] is None else jnp.maximum(tops[u], top)
            for q in range(2):
                turned_back = jnp.transpose(folded[q * LANES : (q + 1) * LANES, :])
                found.append(jnp.max(turned_back, axis=0, keepdims=True))
        both = jnp.broadcast_to(found[0], sub.shape)
        for u, row in enumerate([*found[1:], *tops]):
            both = jnp.where(sub == u + 1, row, both)
        both = 1.0 - both / size
        owner = jnp.where(
            sub < QUARTERS, jnp.full(sub.shape, row_block), jnp.full(sub.shape, col_block)
        )
        for b in range(n):
            best[b] = jnp.minimum(best[b], jnp.where(owner == b, both, EMPTY_VALUE))

    build(0)
    for t in range(len(tiles)):
        if t + 1 < len(tiles):
            build(t + 1)
        product(t)

    if planes > 1:
        pl.semaphore_wait(plane_sem, len_devices - 1)
    for step in sorted(range(1, planes * n), key=lambda s: (s % n, s), reverse=True):
        copy_to(
            best.at[partner(me, step % n, n)],
            parts.at[my_plane * n + step % n],
            send_sem,
            recv_sem,
            len=partner(my_len, step // n, len_devices),
            tile=partner(me, step % n, n),
        ).start()
    parts[my_plane * n] = best[me]
    everyone = parts.at[pl.ds(0, planes * n - 1)]
    await_all(everyone, send_sem, True)
    await_all(everyone, recv_sem, False)
    for g in range(planes):
        for e in range(share):
            merged = parts[g * n + e]
            for step in range(e + share, n, share):
                merged = jnp.minimum(merged, parts[g * n + step])
            l = partner(turn_of_mine, e, share)
            if planes > 1:
                groups[g, l] = merged
            else:
                mine[l] = merged
                groups[my_len, l] = merged
    if planes == 1:
        hops = [
            copy_to(
                mine,
                groups.at[my_len],
                send_len.at[step],
                recv_len.at[step],
                len=partner(my_len, step, len_devices),
            )
            for step in range(1, len_devices)
        ]
        for copy in hops:
            copy.start()
        for copy in hops:
            copy.wait()


def write_kernel(groups_ref, right_ref, left_ref, right, left, sems):
    len_devices, count_len = groups_ref.shape[:2]
    for g in range(len_devices):
        for l in range(count_len):
            row = g * count_len + l
            for u in range(QUARTERS):
                lanes = slice(u * LANES, (u + 1) * LANES)
                right[row : row + 1, lanes] = groups_ref[g, l, u : u + 1, :]
                left[row : row + 1, lanes] = groups_ref[g, l, QUARTERS + u : QUARTERS + u + 1, :]
    copies = [
        pltpu.make_async_copy(right, right_ref, sems.at[0]),
        pltpu.make_async_copy(left, left_ref, sems.at[1]),
    ]
    for copy in copies:
        copy.start()
    for copy in copies:
        copy.wait()


def shards(series, window_lengths, exclusion, tile_list):
    n = lax.axis_size("tile")
    len_devices = lax.axis_size("len")
    count_len = window_lengths.shape[0]
    piece = series.shape[0]
    points = piece * n
    columns = points // LANES
    blocks = (points - MAX_LEN) // TILE_SIDE
    assert blocks == n
    slot_rows = (piece + 2 * LANES - 2) // LANES
    slot_rows = (slot_rows + SUBLANES - 1) // SUBLANES * SUBLANES
    depth = (columns, 1, LANES)
    chunk = next(g for g in range(1, n + 1) if n % g == 0 and g * piece % LANES == 0)
    per = chunk * piece // LANES
    chunk_rows = (per + SUBLANES - 1) // SUBLANES * SUBLANES
    planes = len_devices if len_devices <= 2 else 1
    share = count_len
    assert n % share == 0 and share & (share - 1) == 0
    dma = pltpu.SemaphoreType.DMA

    groups = pl.pallas_call(
        functools.partial(
            profile_kernel,
            piece,
            n,
            count_len,
            len_devices,
            planes,
            chunk,
        ),
        out_shape=pltpu.VMEM((len_devices, count_len, SUBLANES, LANES), jnp.float32),
        in_specs=[pl.BlockSpec(memory_space=HBM)] * 4,
        out_specs=pl.BlockSpec(memory_space=VMEM),
        scratch_shapes=[
            pltpu.VMEM((piece,), jnp.float32),
            pltpu.SMEM((share, *tile_list.shape[::-1]), jnp.int32),
            pltpu.SMEM(window_lengths.shape, jnp.int32),
            pltpu.SMEM(exclusion.shape, jnp.int32),
            pltpu.VMEM((slot_rows * LANES,), jnp.float32),
            pltpu.VMEM((slot_rows, LANES), jnp.float32),
            pltpu.VMEM((n, slot_rows, LANES), jnp.float32),
            pltpu.VMEM((n // chunk, chunk_rows, LANES), jnp.float32),
            pltpu.VMEM((columns, LANES), jnp.float32),
            pltpu.VMEM((columns + 1, LANES, LANES), jnp.float32),
            pltpu.VMEM(depth, jnp.float32),
            pltpu.VMEM(depth, jnp.float32),
            pltpu.VMEM((MAX_LEN, 2 * LANES), jnp.bfloat16),
            pltpu.VMEM((share * tile_list.shape[0], MAX_LEN, TILE_SIDE), jnp.bfloat16),
            pltpu.VMEM((share * tile_list.shape[0], MAX_LEN, TILE_SIDE), jnp.bfloat16),
            pltpu.VMEM((n, SUBLANES, LANES), jnp.float32),
            pltpu.VMEM((planes * n, SUBLANES, LANES), jnp.float32),
            pltpu.VMEM((count_len, SUBLANES, LANES), jnp.float32),
            dma((4,)),
            dma((share,)),
            dma((share,)),
            pltpu.SemaphoreType.REGULAR,
            dma,
            dma((n // chunk,)),
            dma,
            dma,
            dma((len_devices,)),
            dma((len_devices,)),
        ],
        compiler_params=pltpu.CompilerParams(
            collective_id=0,
            has_side_effects=True,
            vmem_limit_bytes=28 * GRANT + points * LANES * 4,
        ),
        name="profile",
    )(
        *(
            pltpu.with_memory_space_constraint(x, HBM)
            for x in (series, tile_list.T, window_lengths, exclusion)
        )
    )

    profile = jax.ShapeDtypeStruct((len_devices * count_len, TILE_SIDE), jnp.float32)
    return pl.pallas_call(
        write_kernel,
        out_shape=(profile, profile),
        in_specs=[pl.BlockSpec(memory_space=VMEM)],
        out_specs=(pl.BlockSpec(memory_space=HBM), pl.BlockSpec(memory_space=HBM)),
        scratch_shapes=[
            pltpu.VMEM(profile.shape, jnp.float32),
            pltpu.VMEM(profile.shape, jnp.float32),
            dma((2,)),
        ],
        compiler_params=pltpu.CompilerParams(vmem_limit_bytes=GRANT),
        name="write_profiles",
    )(groups)


def solution(mesh):
    return jax.shard_map(
        shards,
        mesh=mesh,
        in_specs=(P("tile"), P("len"), P("len"), P("tile", None)),
        out_specs=(P(None, "tile"), P(None, "tile")),
        check_vma=False,
    )
```

```python
import functools

import jax
import jax.numpy as jnp
from jax import lax
from jax.experimental import pallas as pl
from jax.experimental.pallas import tpu as pltpu
from jax.sharding import PartitionSpec as P

MAX_LEN = 1024
TILE_SIDE = 512
LANES = 128
SUBLANES = 8
GRANT = 1 << 20
QUARTERS = TILE_SIDE // LANES

EMPTY_VALUE = 2.0
CLOSED = -1e30
VAR_EPS = 1e-05

VMEM = pltpu.MemorySpace.VMEM
SMEM = pltpu.MemorySpace.SMEM
HBM = pltpu.MemorySpace.HBM


def partner(me, step, n):
    peer = me
    for b in range(n.bit_length() - 1):
        if step >> b & 1:
            peer = peer + (1 << b) * (1 - 2 * lax.rem(lax.div(me, 1 << b), 2))
    return peer


def signal_all(barrier, axis, n):
    for step in range(n - 1, 0, -1):
        pl.semaphore_signal(
            barrier,
            inc=1,
            device_id={axis: partner(lax.axis_index(axis), step, n)},
            device_id_type=pl.DeviceIdType.MESH,
        )


def await_all(ref, sem, sent):
    copy = copy_to(ref, ref, sem, sem)
    copy.wait_send() if sent else copy.wait_recv()


def copy_to(source, target, send_sem, recv_sem, **peer):
    return pltpu.make_async_remote_copy(
        src_ref=source,
        dst_ref=target,
        send_sem=send_sem,
        recv_sem=recv_sem,
        device_id=peer,
        device_id_type=pl.DeviceIdType.MESH,
    )


def shifted(values, count):
    rows = values.shape[0]
    skip, shift = count // LANES, count % LANES
    if shift:
        lane_ids = lax.broadcasted_iota(jnp.int32, values.shape, 1)
        values = pltpu.roll(values, LANES - shift, 1)
        values = jnp.where(lane_ids < LANES - shift, values, pltpu.roll(values, rows - 1, 0))
    if skip:
        values = pltpu.roll(values, rows - skip, 0)
    return values


def window_stats(packed, lengths):
    mean, spread = packed, jnp.zeros_like(packed)
    results = [(jnp.zeros_like(packed), jnp.zeros_like(packed)) for _ in lengths]
    bits = MAX_LEN.bit_length()
    for b in range(bits):
        first = 1 << b
        for l, length in enumerate(lengths):
            tail_mean, tail_spread = results[l]
            if b:
                tail_mean, tail_spread = shifted(tail_mean, first), shifted(tail_spread, first)
            rest = lax.rem(length, first).astype(jnp.float32)
            share = rest / (rest + first)
            gap = tail_mean - mean
            taken = (jnp.full(packed.shape, length) & first) != 0
            results[l] = (
                jnp.where(taken, mean + gap * share, results[l][0]),
                jnp.where(
                    taken, spread + tail_spread + gap * gap * (share * first), results[l][1]
                ),
            )
        if b < bits - 1:
            next_mean = shifted(mean, first)
            gap = next_mean - mean
            mean = 0.5 * (mean + next_mean)
            if b:
                spread = spread + shifted(spread, first) + gap * gap * (0.5 * first)
            else:
                spread = gap * gap * 0.5
    return [
        (mean, 1.0 / jnp.sqrt(spread / length.astype(jnp.float32) + VAR_EPS))
        for (mean, spread), length in zip(results, lengths)
    ]


def profile_kernel(
    piece,
    n,
    count_len,
    len_devices,
    planes,
    chunk,
    series_ref,
    tile_hbm,
    length_hbm,
    barrier_hbm,
    groups,
    piece_ref,
    tile_ref,
    length_ref,
    barrier_ref,
    flat,
    staged,
    slots,
    chunk_rows,
    packed,
    base,
    centre_ref,
    inverse_ref,
    keep_ref,
    bound_ref,
    left_op,
    right_op,
    best,
    parts,
    mine,
    in_sem,
    send_tile,
    recv_tile,
    plane_sem,
    send_piece,
    recv_piece,
    send_sem,
    recv_sem,
    send_len,
    recv_len,
):
    me = lax.axis_index("tile")
    my_len = lax.axis_index("len")
    my_plane = my_len if planes > 1 else 0
    loads = [
        pltpu.make_async_copy(source, target, in_sem.at[k])
        for k, (source, target) in enumerate(
            (
                (series_ref, piece_ref),
                (tile_hbm, tile_ref.at[0]),
                (length_hbm, length_ref),
                (barrier_hbm, barrier_ref),
            )
        )
    ]
    loads[0].start()
    barrier = pltpu.get_barrier_semaphore()
    signal_all(barrier, "tile", n)
    signal_all(barrier, "len", len_devices)
    for load in loads[1:]:
        load.start()

    slot_rows = staged.shape[0]
    flat[...] = jnp.zeros(flat.shape, jnp.float32)
    loads[0].wait()
    flat[:piece] = piece_ref[...]
    values = flat[...].reshape(slot_rows, LANES)
    shift = lax.rem(me * piece, LANES)
    lane_ids = lax.broadcasted_iota(jnp.int32, values.shape, 1)
    values = pltpu.roll(values, shift, 1)
    staged[...] = jnp.where(lane_ids >= shift, values, pltpu.roll(values, 1, 0))

    pl.semaphore_wait(barrier, n - 1 + len_devices - 1)
    for step in range(n - 1, 0, -1):
        copy_to(
            staged,
            slots.at[me],
            send_piece,
            recv_piece.at[step // chunk],
            tile=partner(me, step, n),
        ).start()
    if planes > 1:
        for step in range(1, len_devices):
            pl.semaphore_signal(
                plane_sem,
                inc=1,
                device_id={"len": partner(my_len, step, len_devices)},
                device_id_type=pl.DeviceIdType.MESH,
            )
    slots[me] = staged[...]
    for load in loads[1:]:
        load.wait()
    share = count_len
    passed = [
        copy_to(
            tile_ref.at[0],
            tile_ref.at[e],
            send_tile.at[e],
            recv_tile.at[e],
            tile=partner(me, e, n),
        )
        for e in range(1, share)
    ]
    for copy in passed:
        copy.start()

    turn_of_mine = lax.rem(me, share)
    length, excluded = length_ref[turn_of_mine], barrier_ref[turn_of_mine]
    size = length.astype(jnp.float32)
    parts_of = MAX_LEN // LANES
    last = lax.div(length - 1, LANES)
    order = [lax.rem(last + 1 + c, parts_of) for c in range(parts_of)]
    row_ids = lax.broadcasted_iota(jnp.int32, (LANES, 2 * LANES), 0)
    row_ids = row_ids + (SUBLANES - 1) - 2 * lax.rem(row_ids, SUBLANES)
    keep_ref[...] = jnp.where(row_ids < length - last * LANES, 1.0, 0.0).astype(jnp.bfloat16)
    best[...] = jnp.full(best.shape, EMPTY_VALUE, jnp.float32)
    lane_less_sub = lax.broadcasted_iota(jnp.int32, (SUBLANES, LANES), 1) - lax.broadcasted_iota(
        jnp.int32, (SUBLANES, LANES), 0
    )
    for e in range(bound_ref.shape[0]):
        open_here = lane_less_sub > excluded + (TILE_SIDE - SUBLANES - e * SUBLANES)
        bound_ref[e] = jnp.where(open_here, -CLOSED, CLOSED)

    sub = lax.broadcasted_iota(jnp.int32, (SUBLANES, LANES), 0)
    lane = lax.broadcasted_iota(jnp.int32, (SUBLANES, LANES), 1)
    spans = [
        (
            LANES + 1 - SUBLANES * (g + 1),
            slice(SUBLANES * g, SUBLANES * (g + 1)),
            lane - sub < LANES + 1 - SUBLANES * (g + 1),
        )
        for g in range(LANES // SUBLANES)
    ]
    per = chunk * piece // LANES
    chunks = n // chunk

    def turn(row):
        row = jnp.broadcast_to(row, (SUBLANES, LANES))
        row = pltpu.roll(row, LANES + 1 - SUBLANES, 1, stride=1, stride_axis=0)
        return [row] + [pltpu.roll(row, LANES - SUBLANES * g, 1) for g in range(1, len(spans))]

    for k in range(chunks):
        q = partner(lax.div(me, chunk), k, chunks)
        coming = chunk if k else chunk - 1
        if coming:
            await_all(slots.at[pl.ds(0, coming)], recv_piece.at[k], False)
        chunk_rows[q] = jnp.zeros(chunk_rows.shape[1:], jnp.float32)
        for t in range(chunk):
            low, first = divmod(t * piece, LANES)
            used = (first + piece + LANES - 1) // LANES
            chunk_rows[q, low : low + used, :] += slots[q * chunk + t, :used, :]
        later = None
        for j in range(per - 1, -1, -1):
            moved = turn(chunk_rows[q, j : j + 1, :])
            column = q * per + j + 1
            for g, (_, rows, here) in enumerate(spans):
                beyond = base[column, rows, :] if later is None else later[g]
                base[column, rows, :] = jnp.where(here, moved[g], beyond)
            later = moved
        for g, (_, rows, here) in enumerate(spans):
            base[q * per, rows, :] = jnp.where(here, base[q * per, rows, :], later[g])

    for copy in passed:
        copy.wait()
    await_all(slots.at[pl.ds(0, n - 1)], send_piece, True)
    for q in range(chunks):
        packed[q * per : (q + 1) * per, :] = chunk_rows[q, :per, :]
    columns = packed.shape[0]
    ((centre, inverse),) = window_stats(packed[...], [length])
    centre_ref[...] = centre.reshape(columns, 1, LANES)
    inverse_ref[...] = inverse.reshape(columns, 1, LANES)

    tiles = [(e, slot) for e in range(share) for slot in range(tile_ref.shape[2])]
    blocks_of = [[tile_ref[e, k, slot] for k in range(2)] for e, slot in tiles]

    gates = {}

    def build(t):
        for k, target in enumerate((left_op, right_op)):
            first = blocks_of[t][k] * QUARTERS
            centre, inverse = (
                jnp.concatenate([source[first + u] for u in range(QUARTERS)], axis=1)
                for source in (centre_ref, inverse_ref)
            )
            if t - 2 in gates:
                centre = centre + jnp.concatenate([gates[t - 2]] * QUARTERS, axis=1)
            for c, span in enumerate(order):
                rows = slice(c * LANES, (c + 1) * LANES)
                values = jnp.concatenate(
                    [base[first + u + span + 1] for u in range(QUARTERS)], axis=1
                )
                scale = inverse
                if k == 0 and c < parts_of - 1:
                    scale = inverse * jnp.where(span < last, 1.0, 0.0)
                normal = ((values - centre) * scale).astype(jnp.bfloat16)
                if k == 0 and c == parts_of - 1:
                    normal = normal * jnp.concatenate([keep_ref[...]] * 2, axis=1)
                target[t, rows, :] = normal

    def product(t):
        row_block, col_block = blocks_of[t]
        apart = jnp.minimum(col_block - row_block, 2) * (TILE_SIDE // SUBLANES)
        tops, found = [None] * QUARTERS, []
        for low in range(0, TILE_SIDE, 2 * LANES):
            values = lax.dot_general(
                left_op[t, :, low : low + 2 * LANES],
                right_op[t],
                (((0,), (0,)), ((), ())),
                preferred_element_type=jnp.float32,
            )
            bounds = [
                jnp.concatenate(
                    [
                        bound_ref[apart + (TILE_SIDE + u * LANES - row) // SUBLANES - 1]
                        for row in range(low, low + 2 * LANES, SUBLANES)
                    ],
                    axis=0,
                )
                for u in range(QUARTERS)
            ]
            folded = None
            for u in range(QUARTERS):
                part = jnp.minimum(values[:, u * LANES : (u + 1) * LANES], bounds[u])
                folded = part if folded is None else jnp.maximum(folded, part)
                top = jnp.max(part.reshape(-1, SUBLANES, LANES), axis=0)
                tops[u] = top if tops[u] is None else jnp.maximum(tops[u], top)
            for q in range(2):
                turned_back = jnp.transpose(folded[q * LANES : (q + 1) * LANES, :])
                found.append(jnp.max(turned_back, axis=0, keepdims=True))
        tops = [jnp.max(top, axis=0, keepdims=True) for top in tops]
        met = functools.reduce(jnp.maximum, [*found, *tops])
        gates[t] = jnp.maximum(met - 1e30, 0.0)
        both = jnp.broadcast_to(found[0], sub.shape)
        for u, row in enumerate([*found[1:], *tops]):
            both = jnp.where(sub == u + 1, row, both)
        both = 1.0 - both / size
        owner = jnp.where(
            sub < QUARTERS, jnp.full(sub.shape, row_block), jnp.full(sub.shape, col_block)
        )
        for b in range(n):
            best[b] = jnp.minimum(best[b], jnp.where(owner == b, both, EMPTY_VALUE))

    build(0)
    for t in range(len(tiles)):
        if t + 1 < len(tiles):
            build(t + 1)
        product(t)

    if planes > 1:
        pl.semaphore_wait(plane_sem, len_devices - 1)
    for step in sorted(range(1, planes * n), key=lambda s: (s % n, s), reverse=True):
        copy_to(
            best.at[partner(me, step % n, n)],
            parts.at[my_plane * n + step % n],
            send_sem,
            recv_sem,
            len=partner(my_len, step // n, len_devices),
            tile=partner(me, step % n, n),
        ).start()
    parts[my_plane * n] = best[me]
    everyone = parts.at[pl.ds(0, planes * n - 1)]
    await_all(everyone, send_sem, True)
    await_all(everyone, recv_sem, False)
    for g in range(planes):
        for e in range(share):
            merged = parts[g * n + e]
            for step in range(e + share, n, share):
                merged = jnp.minimum(merged, parts[g * n + step])
            l = partner(turn_of_mine, e, share)
            if planes > 1:
                groups[g, l] = merged
            else:
                mine[l] = merged
                groups[my_len, l] = merged
    if planes == 1:
        hops = [
            copy_to(
                mine,
                groups.at[my_len],
                send_len.at[step],
                recv_len.at[step],
                len=partner(my_len, step, len_devices),
            )
            for step in range(1, len_devices)
        ]
        for copy in hops:
            copy.start()
        for copy in hops:
            copy.wait()


def write_kernel(groups_ref, right_ref, left_ref, right, left, sems):
    len_devices, count_len = groups_ref.shape[:2]
    for g in range(len_devices):
        for l in range(count_len):
            row = g * count_len + l
            for u in range(QUARTERS):
                lanes = slice(u * LANES, (u + 1) * LANES)
                right[row : row + 1, lanes] = groups_ref[g, l, u : u + 1, :]
                left[row : row + 1, lanes] = groups_ref[g, l, QUARTERS + u : QUARTERS + u + 1, :]
    copies = [
        pltpu.make_async_copy(right, right_ref, sems.at[0]),
        pltpu.make_async_copy(left, left_ref, sems.at[1]),
    ]
    for copy in copies:
        copy.start()
    for copy in copies:
        copy.wait()


def shards(series, window_lengths, exclusion, tile_list):
    n = lax.axis_size("tile")
    len_devices = lax.axis_size("len")
    count_len = window_lengths.shape[0]
    piece = series.shape[0]
    points = piece * n
    columns = points // LANES
    blocks = (points - MAX_LEN) // TILE_SIDE
    assert blocks == n
    slot_rows = (piece + 2 * LANES - 2) // LANES
    slot_rows = (slot_rows + SUBLANES - 1) // SUBLANES * SUBLANES
    depth = (columns, 1, LANES)
    chunk = next(g for g in range(1, n + 1) if n % g == 0 and g * piece % LANES == 0)
    per = chunk * piece // LANES
    chunk_rows = (per + SUBLANES - 1) // SUBLANES * SUBLANES
    planes = len_devices if len_devices <= 2 else 1
    bounds = (4 * TILE_SIDE - LANES) // SUBLANES
    share = count_len
    assert n % share == 0 and share & (share - 1) == 0
    dma = pltpu.SemaphoreType.DMA

    groups = pl.pallas_call(
        functools.partial(
            profile_kernel,
            piece,
            n,
            count_len,
            len_devices,
            planes,
            chunk,
        ),
        out_shape=pltpu.VMEM((len_devices, count_len, SUBLANES, LANES), jnp.float32),
        in_specs=[pl.BlockSpec(memory_space=HBM)] * 4,
        out_specs=pl.BlockSpec(memory_space=VMEM),
        scratch_shapes=[
            pltpu.VMEM((piece,), jnp.float32),
            pltpu.SMEM((share, *tile_list.shape[::-1]), jnp.int32),
            pltpu.SMEM(window_lengths.shape, jnp.int32),
            pltpu.SMEM(exclusion.shape, jnp.int32),
            pltpu.VMEM((slot_rows * LANES,), jnp.float32),
            pltpu.VMEM((slot_rows, LANES), jnp.float32),
            pltpu.VMEM((n, slot_rows, LANES), jnp.float32),
            pltpu.VMEM((n // chunk, chunk_rows, LANES), jnp.float32),
            pltpu.VMEM((columns, LANES), jnp.float32),
            pltpu.VMEM((columns + 1, LANES, LANES), jnp.float32),
            pltpu.VMEM(depth, jnp.float32),
            pltpu.VMEM(depth, jnp.float32),
            pltpu.VMEM((LANES, 2 * LANES), jnp.bfloat16),
            pltpu.VMEM((bounds, SUBLANES, LANES), jnp.float32),
            pltpu.VMEM((share * tile_list.shape[0], MAX_LEN, TILE_SIDE), jnp.bfloat16),
            pltpu.VMEM((share * tile_list.shape[0], MAX_LEN, TILE_SIDE), jnp.bfloat16),
            pltpu.VMEM((n, SUBLANES, LANES), jnp.float32),
            pltpu.VMEM((planes * n, SUBLANES, LANES), jnp.float32),
            pltpu.VMEM((count_len, SUBLANES, LANES), jnp.float32),
            dma((4,)),
            dma((share,)),
            dma((share,)),
            pltpu.SemaphoreType.REGULAR,
            dma,
            dma((n // chunk,)),
            dma,
            dma,
            dma((len_devices,)),
            dma((len_devices,)),
        ],
        compiler_params=pltpu.CompilerParams(
            collective_id=0,
            has_side_effects=True,
            vmem_limit_bytes=28 * GRANT + points * LANES * 4,
        ),
        name="profile",
    )(
        *(
            pltpu.with_memory_space_constraint(x, HBM)
            for x in (series, tile_list.T, window_lengths, exclusion)
        )
    )

    profile = jax.ShapeDtypeStruct((len_devices * count_len, TILE_SIDE), jnp.float32)
    return pl.pallas_call(
        write_kernel,
        out_shape=(profile, profile),
        in_specs=[pl.BlockSpec(memory_space=VMEM)],
        out_specs=(pl.BlockSpec(memory_space=HBM), pl.BlockSpec(memory_space=HBM)),
        scratch_shapes=[
            pltpu.VMEM(profile.shape, jnp.float32),
            pltpu.VMEM(profile.shape, jnp.float32),
            dma((2,)),
        ],
        compiler_params=pltpu.CompilerParams(vmem_limit_bytes=GRANT),
        name="write_profiles",
    )(groups)


def solution(mesh):
    return jax.shard_map(
        shards,
        mesh=mesh,
        in_specs=(P("tile"), P("len"), P("len"), P("tile", None)),
        out_specs=(P(None, "tile"), P(None, "tile")),
        check_vma=False,
    )
```

```python
import functools

import jax
import jax.numpy as jnp
from jax import lax
from jax.experimental import pallas as pl
from jax.experimental.pallas import tpu as pltpu
from jax.sharding import PartitionSpec as P

MAX_LEN = 1024
TILE_SIDE = 512
LANES = 128
SUBLANES = 8
GRANT = 1 << 20
QUARTERS = TILE_SIDE // LANES

EMPTY_VALUE = 2.0
CLOSED = -1e30
VAR_EPS = 1e-05

VMEM = pltpu.MemorySpace.VMEM
SMEM = pltpu.MemorySpace.SMEM
HBM = pltpu.MemorySpace.HBM


def partner(me, step, n):
    peer = me
    for b in range(n.bit_length() - 1):
        if step >> b & 1:
            peer = peer + (1 << b) * (1 - 2 * lax.rem(lax.div(me, 1 << b), 2))
    return peer


def signal_all(barrier, axis, n):
    for step in range(n - 1, 0, -1):
        pl.semaphore_signal(
            barrier,
            inc=1,
            device_id={axis: partner(lax.axis_index(axis), step, n)},
            device_id_type=pl.DeviceIdType.MESH,
        )


def await_all(ref, sem, sent):
    copy = copy_to(ref, ref, sem, sem)
    copy.wait_send() if sent else copy.wait_recv()


def copy_to(source, target, send_sem, recv_sem, **peer):
    return pltpu.make_async_remote_copy(
        src_ref=source,
        dst_ref=target,
        send_sem=send_sem,
        recv_sem=recv_sem,
        device_id=peer,
        device_id_type=pl.DeviceIdType.MESH,
    )


def shifted(values, count):
    rows = values.shape[0]
    skip, shift = count // LANES, count % LANES
    if shift:
        lane_ids = lax.broadcasted_iota(jnp.int32, values.shape, 1)
        values = pltpu.roll(values, LANES - shift, 1)
        values = jnp.where(lane_ids < LANES - shift, values, pltpu.roll(values, rows - 1, 0))
    if skip:
        values = pltpu.roll(values, rows - skip, 0)
    return values


def window_stats(packed, lengths):
    mean, spread = packed, jnp.zeros_like(packed)
    results = [(jnp.zeros_like(packed), jnp.zeros_like(packed)) for _ in lengths]
    bits = MAX_LEN.bit_length()
    for b in range(bits):
        first = 1 << b
        for l, length in enumerate(lengths):
            tail_mean, tail_spread = results[l]
            if b:
                tail_mean, tail_spread = shifted(tail_mean, first), shifted(tail_spread, first)
            rest = lax.rem(length, first).astype(jnp.float32)
            share = rest / (rest + first)
            gap = tail_mean - mean
            taken = (jnp.full(packed.shape, length) & first) != 0
            results[l] = (
                jnp.where(taken, mean + gap * share, results[l][0]),
                jnp.where(
                    taken, spread + tail_spread + gap * gap * (share * first), results[l][1]
                ),
            )
        if b < bits - 1:
            next_mean = shifted(mean, first)
            gap = next_mean - mean
            mean = 0.5 * (mean + next_mean)
            if b:
                spread = spread + shifted(spread, first) + gap * gap * (0.5 * first)
            else:
                spread = gap * gap * 0.5
    return [
        (mean, 1.0 / jnp.sqrt(spread / length.astype(jnp.float32) + VAR_EPS))
        for (mean, spread), length in zip(results, lengths)
    ]


def profile_kernel(
    piece,
    n,
    count_len,
    len_devices,
    planes,
    chunk,
    series_ref,
    tile_hbm,
    length_hbm,
    barrier_hbm,
    groups,
    piece_ref,
    tile_ref,
    length_ref,
    barrier_ref,
    flat,
    staged,
    slots,
    chunk_rows,
    packed,
    base,
    centre_ref,
    inverse_ref,
    keep_ref,
    bound_ref,
    left_op,
    right_op,
    best,
    parts,
    mine,
    in_sem,
    send_tile,
    recv_tile,
    plane_sem,
    send_piece,
    recv_piece,
    send_sem,
    recv_sem,
    send_len,
    recv_len,
):
    me = lax.axis_index("tile")
    my_len = lax.axis_index("len")
    my_plane = my_len if planes > 1 else 0
    loads = [
        pltpu.make_async_copy(source, target, in_sem.at[k])
        for k, (source, target) in enumerate(
            (
                (series_ref, piece_ref),
                (tile_hbm, tile_ref.at[0]),
                (length_hbm, length_ref),
                (barrier_hbm, barrier_ref),
            )
        )
    ]
    loads[0].start()
    barrier = pltpu.get_barrier_semaphore()
    signal_all(barrier, "tile", n)
    signal_all(barrier, "len", len_devices)
    for load in loads[1:]:
        load.start()

    slot_rows = staged.shape[0]
    used_rows = max(-(-(t * piece % LANES + piece) // LANES) for t in range(n))
    flat[...] = jnp.zeros(flat.shape, jnp.float32)
    loads[0].wait()
    flat[:piece] = piece_ref[...]
    values = flat[...].reshape(slot_rows, LANES)
    shift = lax.rem(me * piece, LANES)
    lane_ids = lax.broadcasted_iota(jnp.int32, values.shape, 1)
    values = pltpu.roll(values, shift, 1)
    staged[...] = jnp.where(lane_ids >= shift, values, pltpu.roll(values, 1, 0))

    pl.semaphore_wait(barrier, n - 1 + len_devices - 1)
    for step in range(n - 1, 0, -1):
        copy_to(
            staged.at[pl.ds(0, used_rows)],
            slots.at[me, pl.ds(0, used_rows)],
            send_piece,
            recv_piece.at[step // chunk],
            tile=partner(me, step, n),
        ).start()
    if planes > 1:
        for step in range(1, len_devices):
            pl.semaphore_signal(
                plane_sem,
                inc=1,
                device_id={"len": partner(my_len, step, len_devices)},
                device_id_type=pl.DeviceIdType.MESH,
            )
    slots[me] = staged[...]
    for load in loads[1:]:
        load.wait()
    share = count_len
    passed = [
        copy_to(
            tile_ref.at[0],
            tile_ref.at[e],
            send_tile.at[e],
            recv_tile.at[e],
            tile=partner(me, e, n),
        )
        for e in range(1, share)
    ]
    for copy in passed:
        copy.start()

    turn_of_mine = lax.rem(me, share)
    length, excluded = length_ref[turn_of_mine], barrier_ref[turn_of_mine]
    size = length.astype(jnp.float32)
    parts_of = MAX_LEN // LANES
    last = lax.div(length - 1, LANES)
    order = [lax.rem(last + 1 + c, parts_of) for c in range(parts_of)]
    row_ids = lax.broadcasted_iota(jnp.int32, (LANES, 2 * LANES), 0)
    row_ids = row_ids + (SUBLANES - 1) - 2 * lax.rem(row_ids, SUBLANES)
    keep_ref[...] = jnp.where(row_ids < length - last * LANES, 1.0, 0.0).astype(jnp.bfloat16)
    best[...] = jnp.full(best.shape, EMPTY_VALUE, jnp.float32)
    lane_less_sub = lax.broadcasted_iota(jnp.int32, (SUBLANES, LANES), 1) - lax.broadcasted_iota(
        jnp.int32, (SUBLANES, LANES), 0
    )
    for e in range(bound_ref.shape[0]):
        open_here = lane_less_sub > excluded + (TILE_SIDE - SUBLANES - e * SUBLANES)
        bound_ref[e] = jnp.where(open_here, -CLOSED, CLOSED)

    sub = lax.broadcasted_iota(jnp.int32, (SUBLANES, LANES), 0)
    lane = lax.broadcasted_iota(jnp.int32, (SUBLANES, LANES), 1)
    spans = [
        (
            LANES + 1 - SUBLANES * (g + 1),
            slice(SUBLANES * g, SUBLANES * (g + 1)),
            lane - sub < LANES + 1 - SUBLANES * (g + 1),
        )
        for g in range(LANES // SUBLANES)
    ]
    per = chunk * piece // LANES
    chunks = n // chunk

    def turn(row):
        row = jnp.broadcast_to(row, (SUBLANES, LANES))
        row = pltpu.roll(row, LANES + 1 - SUBLANES, 1, stride=1, stride_axis=0)
        return [row] + [pltpu.roll(row, LANES - SUBLANES * g, 1) for g in range(1, len(spans))]

    for k in range(chunks):
        q = partner(lax.div(me, chunk), k, chunks)
        coming = chunk if k else chunk - 1
        if coming:
            await_all(slots.at[pl.ds(0, coming), pl.ds(0, used_rows)], recv_piece.at[k], False)
        chunk_rows[q] = jnp.zeros(chunk_rows.shape[1:], jnp.float32)
        for t in range(chunk):
            low, first = divmod(t * piece, LANES)
            used = (first + piece + LANES - 1) // LANES
            chunk_rows[q, low : low + used, :] += slots[q * chunk + t, :used, :]
        later = None
        for j in range(per - 1, -1, -1):
            moved = turn(chunk_rows[q, j : j + 1, :])
            column = q * per + j + 1
            for g, (_, rows, here) in enumerate(spans):
                beyond = base[column, rows, :] if later is None else later[g]
                base[column, rows, :] = jnp.where(here, moved[g], beyond)
            later = moved
        for g, (_, rows, here) in enumerate(spans):
            base[q * per, rows, :] = jnp.where(here, base[q * per, rows, :], later[g])

    for copy in passed:
        copy.wait()
    await_all(slots.at[pl.ds(0, n - 1), pl.ds(0, used_rows)], send_piece, True)
    for q in range(chunks):
        packed[q * per : (q + 1) * per, :] = chunk_rows[q, :per, :]
    columns = packed.shape[0]
    ((centre, inverse),) = window_stats(packed[...], [length])
    centre_ref[...] = centre.reshape(columns, 1, LANES)
    inverse_ref[...] = inverse.reshape(columns, 1, LANES)

    tiles = [(e, slot) for e in range(share) for slot in range(tile_ref.shape[2])]
    blocks_of = [[tile_ref[e, k, slot] for k in range(2)] for e, slot in tiles]

    gates = {}

    def build(t):
        for k, target in enumerate((left_op, right_op)):
            first = blocks_of[t][k] * QUARTERS
            centre, inverse = (
                jnp.concatenate([source[first + u] for u in range(QUARTERS)], axis=1)
                for source in (centre_ref, inverse_ref)
            )
            if t - 2 in gates:
                centre = centre + jnp.concatenate([gates[t - 2][k]] * QUARTERS, axis=1)
            for c, span in enumerate(order):
                rows = slice(c * LANES, (c + 1) * LANES)
                values = jnp.concatenate(
                    [base[first + u + span + 1] for u in range(QUARTERS)], axis=1
                )
                scale = inverse
                if k == 0 and c < parts_of - 1:
                    scale = inverse * jnp.where(span < last, 1.0, 0.0)
                normal = ((values - centre) * scale).astype(jnp.bfloat16)
                if k == 0 and c == parts_of - 1:
                    normal = normal * jnp.concatenate([keep_ref[...]] * 2, axis=1)
                target[t, rows, :] = normal

    half = TILE_SIDE // 2

    def product(t, row, col, width):
        row_block, col_block = blocks_of[t]
        apart = jnp.minimum(col_block - row_block, 2) * (TILE_SIDE // SUBLANES)
        values = lax.dot_general(
            left_op[t, :, row : row + half],
            right_op[t, :, col : col + width],
            (((0,), (0,)), ((), ())),
            preferred_element_type=jnp.float32,
        )
        folded, tops = None, []
        for u in range(0, width, LANES):
            bounds = jnp.concatenate(
                [
                    bound_ref[apart + (TILE_SIDE + col + u - line) // SUBLANES - 1]
                    for line in range(row, row + half, SUBLANES)
                ],
                axis=0,
            )
            part = jnp.minimum(values[:, u : u + LANES], bounds)
            folded = part if folded is None else jnp.maximum(folded, part)
            tops.append(jnp.max(part.reshape(-1, SUBLANES, LANES), axis=0))
        found = [
            jnp.max(jnp.transpose(folded[u : u + LANES, :]), axis=0, keepdims=True)
            for u in range(0, half, LANES)
        ]
        return found, tops

    def larger(some, others):
        return [jnp.maximum(x, y) for x, y in zip(some, others)]

    lines4 = lax.broadcasted_iota(jnp.int32, (QUARTERS, LANES), 0)

    def update(r, t, right, left):
        row_block, col_block = blocks_of[t]
        left = [jnp.max(top, axis=0, keepdims=True) for top in left]
        both = jnp.broadcast_to(right[0], lines4.shape)
        for u, line in enumerate([*right[1:], *left]):
            both = jnp.where(lines4 == u + 1, line, both)
        both = 1.0 - both / size
        owner = jnp.where(
            lines4 < len(right),
            jnp.full(lines4.shape, row_block),
            jnp.full(lines4.shape, col_block),
        )
        for b in range(n):
            best[r, b] = jnp.minimum(best[r, b], jnp.where(owner == b, both, EMPTY_VALUE))
        return jnp.maximum(functools.reduce(jnp.maximum, [*right, *left]) - 1e30, 0.0)

    def send(r):
        for step in sorted(range(1, planes * n), key=lambda s: (s % n, s), reverse=True):
            copy_to(
                best.at[r, partner(me, step % n, n)],
                parts.at[r, my_plane * n + step % n],
                send_sem.at[r],
                recv_sem.at[r],
                len=partner(my_len, step // n, len_devices),
                tile=partner(me, step % n, n),
            ).start()
        parts[r, my_plane * n] = best[r, me]

    kept = {}
    build(0)
    for t in range(len(tiles)):
        if t + 1 < len(tiles):
            build(t + 1)
        found, tops = product(t, 0, 0, TILE_SIDE)
        found_below, tops_below = product(t, half, 0, half)
        gates[t] = (
            jnp.maximum(found[0] - 1e30, 0.0),
            update(0, t, found, larger(tops[:2], tops_below)),
        )
        kept[t] = found_below, tops[2:]
    if planes > 1:
        pl.semaphore_wait(plane_sem, len_devices - 1)
    send(0)
    for t in range(len(tiles)):
        found, tops = product(t, half, half, half)
        found_before, tops_before = kept[t]
        update(1, t, larger(found, found_before), larger(tops, tops_before))
    send(1)

    everyone = parts.at[0, pl.ds(0, planes * n - 1)]
    for r in range(2):
        await_all(everyone, send_sem.at[r], True)
    for r in range(2):
        await_all(everyone, recv_sem.at[r], False)
        for g in range(planes):
            for e in range(share):
                merged = parts[r, g * n + e]
                for step in range(e + share, n, share):
                    merged = jnp.minimum(merged, parts[r, g * n + step])
                l = partner(turn_of_mine, e, share)
                if planes > 1:
                    groups[g, l, r] = merged
                else:
                    mine[l, r] = merged
                    groups[my_len, l, r] = merged
    if planes == 1:
        hops = [
            copy_to(
                mine,
                groups.at[my_len],
                send_len.at[step],
                recv_len.at[step],
                len=partner(my_len, step, len_devices),
            )
            for step in range(1, len_devices)
        ]
        for copy in hops:
            copy.start()
        for copy in hops:
            copy.wait()


def write_kernel(groups_ref, right_ref, left_ref, right, left, sems):
    len_devices, count_len = groups_ref.shape[:2]
    for g in range(len_devices):
        for l in range(count_len):
            row = g * count_len + l
            for u in range(QUARTERS):
                lanes = slice(u * LANES, (u + 1) * LANES)
                line = u % 2
                right[row : row + 1, lanes] = groups_ref[g, l, u // 2, line : line + 1, :]
                left[row : row + 1, lanes] = groups_ref[g, l, u // 2, line + 2 : line + 3, :]
    copies = [
        pltpu.make_async_copy(right, right_ref, sems.at[0]),
        pltpu.make_async_copy(left, left_ref, sems.at[1]),
    ]
    for copy in copies:
        copy.start()
    for copy in copies:
        copy.wait()


def shards(series, window_lengths, exclusion, tile_list):
    n = lax.axis_size("tile")
    len_devices = lax.axis_size("len")
    count_len = window_lengths.shape[0]
    piece = series.shape[0]
    points = piece * n
    columns = points // LANES
    blocks = (points - MAX_LEN) // TILE_SIDE
    assert blocks == n
    slot_rows = (piece + 2 * LANES - 2) // LANES
    slot_rows = (slot_rows + SUBLANES - 1) // SUBLANES * SUBLANES
    depth = (columns, 1, LANES)
    chunk = next(g for g in range(1, n + 1) if n % g == 0 and g * piece % LANES == 0)
    per = chunk * piece // LANES
    chunk_rows = (per + SUBLANES - 1) // SUBLANES * SUBLANES
    planes = len_devices if len_devices <= 2 else 1
    bounds = (4 * TILE_SIDE - LANES) // SUBLANES
    share = count_len
    assert n % share == 0 and share & (share - 1) == 0
    dma = pltpu.SemaphoreType.DMA

    groups = pl.pallas_call(
        functools.partial(
            profile_kernel,
            piece,
            n,
            count_len,
            len_devices,
            planes,
            chunk,
        ),
        out_shape=pltpu.VMEM((len_devices, count_len, 2, QUARTERS, LANES), jnp.float32),
        in_specs=[pl.BlockSpec(memory_space=HBM)] * 4,
        out_specs=pl.BlockSpec(memory_space=VMEM),
        scratch_shapes=[
            pltpu.VMEM((piece,), jnp.float32),
            pltpu.SMEM((share, *tile_list.shape[::-1]), jnp.int32),
            pltpu.SMEM(window_lengths.shape, jnp.int32),
            pltpu.SMEM(exclusion.shape, jnp.int32),
            pltpu.VMEM((slot_rows * LANES,), jnp.float32),
            pltpu.VMEM((slot_rows, LANES), jnp.float32),
            pltpu.VMEM((n, slot_rows, LANES), jnp.float32),
            pltpu.VMEM((n // chunk, chunk_rows, LANES), jnp.float32),
            pltpu.VMEM((columns, LANES), jnp.float32),
            pltpu.VMEM((columns + 1, LANES, LANES), jnp.float32),
            pltpu.VMEM(depth, jnp.float32),
            pltpu.VMEM(depth, jnp.float32),
            pltpu.VMEM((LANES, 2 * LANES), jnp.bfloat16),
            pltpu.VMEM((bounds, SUBLANES, LANES), jnp.float32),
            pltpu.VMEM((share * tile_list.shape[0], MAX_LEN, TILE_SIDE), jnp.bfloat16),
            pltpu.VMEM((share * tile_list.shape[0], MAX_LEN, TILE_SIDE), jnp.bfloat16),
            pltpu.VMEM((2, n, QUARTERS, LANES), jnp.float32),
            pltpu.VMEM((2, planes * n, QUARTERS, LANES), jnp.float32),
            pltpu.VMEM((count_len, 2, QUARTERS, LANES), jnp.float32),
            dma((4,)),
            dma((share,)),
            dma((share,)),
            pltpu.SemaphoreType.REGULAR,
            dma,
            dma((n // chunk,)),
            dma((2,)),
            dma((2,)),
            dma((len_devices,)),
            dma((len_devices,)),
        ],
        compiler_params=pltpu.CompilerParams(
            collective_id=0,
            has_side_effects=True,
            vmem_limit_bytes=28 * GRANT + points * LANES * 4,
        ),
        name="profile",
    )(
        *(
            pltpu.with_memory_space_constraint(x, HBM)
            for x in (series, tile_list.T, window_lengths, exclusion)
        )
    )

    profile = jax.ShapeDtypeStruct((len_devices * count_len, TILE_SIDE), jnp.float32)
    return pl.pallas_call(
        write_kernel,
        out_shape=(profile, profile),
        in_specs=[pl.BlockSpec(memory_space=VMEM)],
        out_specs=(pl.BlockSpec(memory_space=HBM), pl.BlockSpec(memory_space=HBM)),
        scratch_shapes=[
            pltpu.VMEM(profile.shape, jnp.float32),
            pltpu.VMEM(profile.shape, jnp.float32),
            dma((2,)),
        ],
        compiler_params=pltpu.CompilerParams(vmem_limit_bytes=GRANT),
        name="write_profiles",
    )(groups)


def solution(mesh):
    return jax.shard_map(
        shards,
        mesh=mesh,
        in_specs=(P("tile"), P("len"), P("len"), P("tile", None)),
        out_specs=(P(None, "tile"), P(None, "tile")),
        check_vma=False,
    )
```

```python
import functools

import jax
import jax.numpy as jnp
from jax import lax
from jax.experimental import pallas as pl
from jax.experimental.pallas import tpu as pltpu
from jax.sharding import PartitionSpec as P

MAX_LEN = 1024
TILE_SIDE = 512
LANES = 128
SUBLANES = 8
GRANT = 1 << 20
QUARTERS = TILE_SIDE // LANES

EMPTY_VALUE = 2.0
CLOSED = -1e30
VAR_EPS = 1e-05

VMEM = pltpu.MemorySpace.VMEM
SMEM = pltpu.MemorySpace.SMEM
HBM = pltpu.MemorySpace.HBM


def partner(me, step, n):
    peer = me
    for b in range(n.bit_length() - 1):
        if step >> b & 1:
            peer = peer + (1 << b) * (1 - 2 * lax.rem(lax.div(me, 1 << b), 2))
    return peer


def signal_all(barrier, axis, n):
    for step in range(n - 1, 0, -1):
        pl.semaphore_signal(
            barrier,
            inc=1,
            device_id={axis: partner(lax.axis_index(axis), step, n)},
            device_id_type=pl.DeviceIdType.MESH,
        )


def await_all(ref, sem, sent):
    copy = copy_to(ref, ref, sem, sem)
    copy.wait_send() if sent else copy.wait_recv()


def copy_to(source, target, send_sem, recv_sem, **peer):
    return pltpu.make_async_remote_copy(
        src_ref=source,
        dst_ref=target,
        send_sem=send_sem,
        recv_sem=recv_sem,
        device_id=peer,
        device_id_type=pl.DeviceIdType.MESH,
    )


def shifted(values, count):
    rows = values.shape[0]
    skip, shift = count // LANES, count % LANES
    if shift:
        lane_ids = lax.broadcasted_iota(jnp.int32, values.shape, 1)
        values = pltpu.roll(values, LANES - shift, 1)
        values = jnp.where(lane_ids < LANES - shift, values, pltpu.roll(values, rows - 1, 0))
    if skip:
        values = pltpu.roll(values, rows - skip, 0)
    return values


def window_stats(packed, lengths):
    mean, spread = packed, jnp.zeros_like(packed)
    results = [(jnp.zeros_like(packed), jnp.zeros_like(packed)) for _ in lengths]
    bits = MAX_LEN.bit_length()
    for b in range(bits):
        first = 1 << b
        for l, length in enumerate(lengths):
            tail_mean, tail_spread = results[l]
            if b:
                tail_mean, tail_spread = shifted(tail_mean, first), shifted(tail_spread, first)
            rest = lax.rem(length, first).astype(jnp.float32)
            share = rest / (rest + first)
            gap = tail_mean - mean
            taken = (jnp.full(packed.shape, length) & first) != 0
            results[l] = (
                jnp.where(taken, mean + gap * share, results[l][0]),
                jnp.where(
                    taken, spread + tail_spread + gap * gap * (share * first), results[l][1]
                ),
            )
        if b < bits - 1:
            next_mean = shifted(mean, first)
            gap = next_mean - mean
            mean = 0.5 * (mean + next_mean)
            if b:
                spread = spread + shifted(spread, first) + gap * gap * (0.5 * first)
            else:
                spread = gap * gap * 0.5
    return [
        (mean, 1.0 / jnp.sqrt(spread / length.astype(jnp.float32) + VAR_EPS))
        for (mean, spread), length in zip(results, lengths)
    ]


def profile_kernel(
    piece,
    n,
    count_len,
    len_devices,
    planes,
    chunk,
    series_ref,
    tile_hbm,
    length_hbm,
    barrier_hbm,
    groups,
    piece_ref,
    tile_ref,
    length_ref,
    barrier_ref,
    flat,
    staged,
    slots,
    chunk_rows,
    packed,
    base,
    centre_ref,
    inverse_ref,
    keep_ref,
    bound_ref,
    left_op,
    right_op,
    best,
    parts,
    mine,
    in_sem,
    send_tile,
    recv_tile,
    plane_sem,
    send_piece,
    recv_piece,
    send_sem,
    recv_sem,
    send_len,
    recv_len,
):
    me = lax.axis_index("tile")
    my_len = lax.axis_index("len")
    my_plane = my_len if planes > 1 else 0
    loads = [
        pltpu.make_async_copy(source, target, in_sem.at[k])
        for k, (source, target) in enumerate(
            (
                (series_ref, piece_ref),
                (tile_hbm, tile_ref.at[0]),
                (length_hbm, length_ref),
                (barrier_hbm, barrier_ref),
            )
        )
    ]
    loads[0].start()
    barrier = pltpu.get_barrier_semaphore()
    signal_all(barrier, "tile", n)
    signal_all(barrier, "len", len_devices)
    for load in loads[1:]:
        load.start()

    slot_rows = staged.shape[0]
    used_rows = max(-(-(t * piece % LANES + piece) // LANES) for t in range(n))
    flat[...] = jnp.zeros(flat.shape, jnp.float32)
    loads[0].wait()
    flat[:piece] = piece_ref[...]
    values = flat[...].reshape(slot_rows, LANES)
    shift = lax.rem(me * piece, LANES)
    lane_ids = lax.broadcasted_iota(jnp.int32, values.shape, 1)
    values = pltpu.roll(values, shift, 1)
    staged[...] = jnp.where(lane_ids >= shift, values, pltpu.roll(values, 1, 0))

    pl.semaphore_wait(barrier, n - 1 + len_devices - 1)
    for step in range(n - 1, 0, -1):
        copy_to(
            staged.at[pl.ds(0, used_rows)],
            slots.at[me, pl.ds(0, used_rows)],
            send_piece,
            recv_piece.at[step // chunk],
            tile=partner(me, step, n),
        ).start()
    if planes > 1:
        for step in range(1, len_devices):
            pl.semaphore_signal(
                plane_sem,
                inc=1,
                device_id={"len": partner(my_len, step, len_devices)},
                device_id_type=pl.DeviceIdType.MESH,
            )
    slots[me] = staged[...]
    for load in loads[1:]:
        load.wait()
    share = count_len
    passed = [
        copy_to(
            tile_ref.at[0],
            tile_ref.at[e],
            send_tile.at[e],
            recv_tile.at[e],
            tile=partner(me, e, n),
        )
        for e in range(1, share)
    ]
    for copy in passed:
        copy.start()

    turn_of_mine = lax.rem(me, share)
    length, excluded = length_ref[turn_of_mine], barrier_ref[turn_of_mine]
    size = length.astype(jnp.float32)
    parts_of = MAX_LEN // LANES
    last = lax.div(length - 1, LANES)
    order = [lax.rem(last + 1 + c, parts_of) for c in range(parts_of)]
    row_ids = lax.broadcasted_iota(jnp.int32, (LANES, 2 * LANES), 0)
    row_ids = row_ids + (SUBLANES - 1) - 2 * lax.rem(row_ids, SUBLANES)
    keep_ref[...] = jnp.where(row_ids < length - last * LANES, 1.0, 0.0).astype(jnp.bfloat16)
    best[...] = jnp.full(best.shape, EMPTY_VALUE, jnp.float32)
    lane_less_sub = lax.broadcasted_iota(jnp.int32, (SUBLANES, LANES), 1) - lax.broadcasted_iota(
        jnp.int32, (SUBLANES, LANES), 0
    )
    for e in range(bound_ref.shape[0]):
        open_here = lane_less_sub > excluded + (TILE_SIDE - SUBLANES - e * SUBLANES)
        bound_ref[e] = jnp.where(open_here, -CLOSED, CLOSED)

    sub = lax.broadcasted_iota(jnp.int32, (SUBLANES, LANES), 0)
    lane = lax.broadcasted_iota(jnp.int32, (SUBLANES, LANES), 1)
    spans = [
        (
            LANES + 1 - SUBLANES * (g + 1),
            slice(SUBLANES * g, SUBLANES * (g + 1)),
            lane - sub < LANES + 1 - SUBLANES * (g + 1),
        )
        for g in range(LANES // SUBLANES)
    ]
    per = chunk * piece // LANES
    chunks = n // chunk

    def turn(row):
        row = jnp.broadcast_to(row, (SUBLANES, LANES))
        row = pltpu.roll(row, LANES + 1 - SUBLANES, 1, stride=1, stride_axis=0)
        return [row] + [pltpu.roll(row, LANES - SUBLANES * g, 1) for g in range(1, len(spans))]

    for k in range(chunks):
        q = partner(lax.div(me, chunk), k, chunks)
        coming = chunk if k else chunk - 1
        if coming:
            await_all(slots.at[pl.ds(0, coming), pl.ds(0, used_rows)], recv_piece.at[k], False)
        chunk_rows[q] = jnp.zeros(chunk_rows.shape[1:], jnp.float32)
        for t in range(chunk):
            low, first = divmod(t * piece, LANES)
            used = (first + piece + LANES - 1) // LANES
            chunk_rows[q, low : low + used, :] += slots[q * chunk + t, :used, :]
        later = None
        for j in range(per - 1, -1, -1):
            moved = turn(chunk_rows[q, j : j + 1, :])
            column = q * per + j + 1
            for g, (_, rows, here) in enumerate(spans):
                beyond = base[column, rows, :] if later is None else later[g]
                base[column, rows, :] = jnp.where(here, moved[g], beyond)
            later = moved
        for g, (_, rows, here) in enumerate(spans):
            base[q * per, rows, :] = jnp.where(here, base[q * per, rows, :], later[g])

    for copy in passed:
        copy.wait()
    await_all(slots.at[pl.ds(0, n - 1), pl.ds(0, used_rows)], send_piece, True)
    for q in range(chunks):
        packed[q * per : (q + 1) * per, :] = chunk_rows[q, :per, :]
    columns = packed.shape[0]
    ((centre, inverse),) = window_stats(packed[...], [length])
    centre_ref[...] = centre.reshape(columns, 1, LANES)
    inverse_ref[...] = inverse.reshape(columns, 1, LANES)

    tiles = [(e, slot) for e in range(share) for slot in range(tile_ref.shape[2])]
    blocks_of = [[tile_ref[e, k, slot] for k in range(2)] for e, slot in tiles]

    gates = {}

    def build(t):
        for k, target in enumerate((left_op, right_op)):
            first = blocks_of[t][k] * QUARTERS
            centre, inverse = (
                jnp.concatenate([source[first + u] for u in range(QUARTERS)], axis=1)
                for source in (centre_ref, inverse_ref)
            )
            if t - 2 in gates:
                centre = centre + jnp.concatenate([gates[t - 2][k]] * QUARTERS, axis=1)
            for c, span in enumerate(order):
                rows = slice(c * LANES, (c + 1) * LANES)
                values = jnp.concatenate(
                    [base[first + u + span + 1] for u in range(QUARTERS)], axis=1
                )
                scale = inverse
                if k == 0 and c < parts_of - 1:
                    scale = inverse * jnp.where(span < last, 1.0, 0.0)
                normal = ((values - centre) * scale).astype(jnp.bfloat16)
                if k == 0 and c == parts_of - 1:
                    normal = normal * jnp.concatenate([keep_ref[...]] * 2, axis=1)
                target[t, rows, :] = normal

    half = TILE_SIDE // 2

    def product(t, row, col, width):
        row_block, col_block = blocks_of[t]
        apart = jnp.minimum(col_block - row_block, 2) * (TILE_SIDE // SUBLANES)
        values = lax.dot_general(
            left_op[t, :, row : row + half],
            right_op[t, :, col : col + width],
            (((0,), (0,)), ((), ())),
            preferred_element_type=jnp.float32,
        )
        folded, tops = None, []
        for u in range(0, width, LANES):
            bounds = jnp.concatenate(
                [
                    bound_ref[apart + (TILE_SIDE + col + u - line) // SUBLANES - 1]
                    for line in range(row, row + half, SUBLANES)
                ],
                axis=0,
            )
            part = jnp.minimum(values[:, u : u + LANES], bounds)
            folded = part if folded is None else jnp.maximum(folded, part)
            tops.append(jnp.max(part.reshape(-1, SUBLANES, LANES), axis=0))
        found = [
            jnp.max(jnp.transpose(folded[u : u + LANES, :]), axis=0, keepdims=True)
            for u in range(0, half, LANES)
        ]
        return found, tops

    def larger(some, others):
        return [jnp.maximum(x, y) for x, y in zip(some, others)]

    lines4 = lax.broadcasted_iota(jnp.int32, (QUARTERS, LANES), 0)

    def update(r, t, right, left):
        row_block, col_block = blocks_of[t]
        left = [jnp.max(top, axis=0, keepdims=True) for top in left]
        both = jnp.broadcast_to(right[0], lines4.shape)
        for u, line in enumerate([*right[1:], *left]):
            both = jnp.where(lines4 == u + 1, line, both)
        both = 1.0 - both / size
        owner = jnp.where(
            lines4 < len(right),
            jnp.full(lines4.shape, row_block),
            jnp.full(lines4.shape, col_block),
        )
        for b in range(n):
            best[r, b] = jnp.minimum(best[r, b], jnp.where(owner == b, both, EMPTY_VALUE))
        return jnp.maximum(functools.reduce(jnp.maximum, [*right, *left]) - 1e30, 0.0)

    def send(r):
        for step in sorted(range(1, planes * n), key=lambda s: (s % n, s), reverse=True):
            copy_to(
                best.at[r, partner(me, step % n, n)],
                parts.at[r, my_plane * n + step % n],
                send_sem.at[r],
                recv_sem.at[r],
                len=partner(my_len, step // n, len_devices),
                tile=partner(me, step % n, n),
            ).start()
        parts[r, my_plane * n] = best[r, me]

    kept = {}
    build(0)
    for t in range(len(tiles)):
        if t + 1 < len(tiles):
            build(t + 1)
        found, tops = product(t, 0, 0, TILE_SIDE)
        found_below, tops_below = product(t, half, 0, half)
        gates[t] = (
            jnp.maximum(found[0] - 1e30, 0.0),
            update(0, t, found, larger(tops[:2], tops_below)),
        )
        kept[t] = found_below, tops[2:]
    if planes > 1:
        pl.semaphore_wait(plane_sem, len_devices - 1)
    send(0)
    for t in range(len(tiles)):
        found, tops = product(t, half, half, half)
        found_before, tops_before = kept[t]
        update(1, t, larger(found, found_before), larger(tops, tops_before))
    send(1)

    everyone = parts.at[0, pl.ds(0, planes * n - 1)]
    for r in range(2):
        await_all(everyone, recv_sem.at[r], False)
        for g in range(planes):
            for e in range(share):
                merged = parts[r, g * n + e]
                for step in range(e + share, n, share):
                    merged = jnp.minimum(merged, parts[r, g * n + step])
                l = partner(turn_of_mine, e, share)
                if planes > 1:
                    groups[g, l, r] = merged
                else:
                    mine[l, r] = merged
                    groups[my_len, l, r] = merged
    for r in range(2):
        await_all(everyone, send_sem.at[r], True)
    if planes == 1:
        hops = [
            copy_to(
                mine,
                groups.at[my_len],
                send_len.at[step],
                recv_len.at[step],
                len=partner(my_len, step, len_devices),
            )
            for step in range(1, len_devices)
        ]
        for copy in hops:
            copy.start()
        for copy in hops:
            copy.wait()


def write_kernel(groups_ref, right_ref, left_ref, right, left, sems):
    len_devices, count_len = groups_ref.shape[:2]
    for g in range(len_devices):
        for l in range(count_len):
            row = g * count_len + l
            for u in range(QUARTERS):
                lanes = slice(u * LANES, (u + 1) * LANES)
                line = u % 2
                right[row : row + 1, lanes] = groups_ref[g, l, u // 2, line : line + 1, :]
                left[row : row + 1, lanes] = groups_ref[g, l, u // 2, line + 2 : line + 3, :]
    copies = [
        pltpu.make_async_copy(right, right_ref, sems.at[0]),
        pltpu.make_async_copy(left, left_ref, sems.at[1]),
    ]
    for copy in copies:
        copy.start()
    for copy in copies:
        copy.wait()


def shards(series, window_lengths, exclusion, tile_list):
    n = lax.axis_size("tile")
    len_devices = lax.axis_size("len")
    count_len = window_lengths.shape[0]
    piece = series.shape[0]
    points = piece * n
    columns = points // LANES
    blocks = (points - MAX_LEN) // TILE_SIDE
    assert blocks == n
    slot_rows = (piece + 2 * LANES - 2) // LANES
    slot_rows = (slot_rows + SUBLANES - 1) // SUBLANES * SUBLANES
    depth = (columns, 1, LANES)
    chunk = next(g for g in range(1, n + 1) if n % g == 0 and g * piece % LANES == 0)
    per = chunk * piece // LANES
    chunk_rows = (per + SUBLANES - 1) // SUBLANES * SUBLANES
    planes = len_devices if len_devices <= 2 else 1
    bounds = (4 * TILE_SIDE - LANES) // SUBLANES
    share = count_len
    assert n % share == 0 and share & (share - 1) == 0
    dma = pltpu.SemaphoreType.DMA

    groups = pl.pallas_call(
        functools.partial(
            profile_kernel,
            piece,
            n,
            count_len,
            len_devices,
            planes,
            chunk,
        ),
        out_shape=pltpu.VMEM((len_devices, count_len, 2, QUARTERS, LANES), jnp.float32),
        in_specs=[pl.BlockSpec(memory_space=HBM)] * 4,
        out_specs=pl.BlockSpec(memory_space=VMEM),
        scratch_shapes=[
            pltpu.VMEM((piece,), jnp.float32),
            pltpu.SMEM((share, *tile_list.shape[::-1]), jnp.int32),
            pltpu.SMEM(window_lengths.shape, jnp.int32),
            pltpu.SMEM(exclusion.shape, jnp.int32),
            pltpu.VMEM((slot_rows * LANES,), jnp.float32),
            pltpu.VMEM((slot_rows, LANES), jnp.float32),
            pltpu.VMEM((n, slot_rows, LANES), jnp.float32),
            pltpu.VMEM((n // chunk, chunk_rows, LANES), jnp.float32),
            pltpu.VMEM((columns, LANES), jnp.float32),
            pltpu.VMEM((columns + 1, LANES, LANES), jnp.float32),
            pltpu.VMEM(depth, jnp.float32),
            pltpu.VMEM(depth, jnp.float32),
            pltpu.VMEM((LANES, 2 * LANES), jnp.bfloat16),
            pltpu.VMEM((bounds, SUBLANES, LANES), jnp.float32),
            pltpu.VMEM((share * tile_list.shape[0], MAX_LEN, TILE_SIDE), jnp.bfloat16),
            pltpu.VMEM((share * tile_list.shape[0], MAX_LEN, TILE_SIDE), jnp.bfloat16),
            pltpu.VMEM((2, n, QUARTERS, LANES), jnp.float32),
            pltpu.VMEM((2, planes * n, QUARTERS, LANES), jnp.float32),
            pltpu.VMEM((count_len, 2, QUARTERS, LANES), jnp.float32),
            dma((4,)),
            dma((share,)),
            dma((share,)),
            pltpu.SemaphoreType.REGULAR,
            dma,
            dma((n // chunk,)),
            dma((2,)),
            dma((2,)),
            dma((len_devices,)),
            dma((len_devices,)),
        ],
        compiler_params=pltpu.CompilerParams(
            collective_id=0,
            has_side_effects=True,
            vmem_limit_bytes=28 * GRANT + points * LANES * 4,
        ),
        name="profile",
    )(
        *(
            pltpu.with_memory_space_constraint(x, HBM)
            for x in (series, tile_list.T, window_lengths, exclusion)
        )
    )

    profile = jax.ShapeDtypeStruct((len_devices * count_len, TILE_SIDE), jnp.float32)
    return pl.pallas_call(
        write_kernel,
        out_shape=(profile, profile),
        in_specs=[pl.BlockSpec(memory_space=VMEM)],
        out_specs=(pl.BlockSpec(memory_space=HBM), pl.BlockSpec(memory_space=HBM)),
        scratch_shapes=[
            pltpu.VMEM(profile.shape, jnp.float32),
            pltpu.VMEM(profile.shape, jnp.float32),
            dma((2,)),
        ],
        compiler_params=pltpu.CompilerParams(vmem_limit_bytes=GRANT),
        name="write_profiles",
    )(groups)


def solution(mesh):
    return jax.shard_map(
        shards,
        mesh=mesh,
        in_specs=(P("tile"), P("len"), P("len"), P("tile", None)),
        out_specs=(P(None, "tile"), P(None, "tile")),
        check_vma=False,
    )
```
